8 devices in a mesh: dp: 2 (over z, y), fsdp: 4 (over x, core).
Axes of the slice: x: 2, y: 2, z: 1, core: 2. Of those that a mesh axis runs over, the one named last changes fastest.
Arguments:
- h_saved: bfloat16 [4, 16, 2048, 896], P(None, ('dp', 'fsdp'))
- grad_out: bfloat16 [16, 2048, 896], P(('dp', 'fsdp'))
- w_gate: bfloat16 [4, 896, 4864], P(None, 'fsdp')
- w_up: bfloat16 [4, 896, 4864], P(None, 'fsdp')
- w_down: bfloat16 [4, 4864, 896], P(None, 'fsdp')
Outputs:
- output 1: float32 [4, 896, 4864], P(None, 'fsdp')
- output 2: float32 [4, 896, 4864], P(None, 'fsdp')
- output 3: float32 [4, 4864, 896], P(None, 'fsdp')
- output 4: bfloat16 [16, 2048, 896], P(('dp', 'fsdp'))
All inputs are finite; a program needn't handle non-finite values.
Results may differ from the reference program's by a relative error of at most 0.00808875.
Values are sent between devices in bfloat16 or wider.
A program may use at most 1 GiB of HBM per device.

```python
import jax
import jax.numpy as jnp
from jax import lax

LAYERS = 4
BATCH_DEV = 2
SEQ = 2048
D = 896
FF = 4864
SHARDS = 8

BATCH = SHARDS * BATCH_DEV
TOK_SHARD = BATCH_DEV * SEQ
EPS = 1e-5


def setup_inputs(seed: int = 0) -> dict:
    keys = jax.random.split(jax.random.key(seed), 5)
    h_saved = jax.random.normal(keys[0], (LAYERS, BATCH, SEQ, D), jnp.float32).astype(jnp.bfloat16)
    grad_out = jax.random.normal(keys[1], (BATCH, SEQ, D), jnp.float32).astype(jnp.bfloat16)
    w_gate = (jax.random.normal(keys[2], (LAYERS, D, FF), jnp.float32) * D ** -0.5).astype(jnp.bfloat16)
    w_up = (jax.random.normal(keys[3], (LAYERS, D, FF), jnp.float32) * D ** -0.5).astype(jnp.bfloat16)
    w_down = (jax.random.normal(keys[4], (LAYERS, FF, D), jnp.float32) * FF ** -0.5).astype(jnp.bfloat16)
    return {"h_saved": h_saved, "grad_out": grad_out, "w_gate": w_gate, "w_up": w_up, "w_down": w_down}


def layer_backward(h_in, g_acc, gate_w, up_w, down_w):
    x_full = h_in.astype(jnp.float32)
    inv_rms = lax.rsqrt(jnp.mean(x_full * x_full, axis=-1, keepdims=True) + EPS)
    norm_f = x_full * inv_rms
    norm_b = norm_f.astype(jnp.bfloat16)
    pre_gate = jnp.dot(norm_b, gate_w, preferred_element_type=jnp.float32)
    pre_up = jnp.dot(norm_b, up_w, preferred_element_type=jnp.float32)
    sig_gate = jax.nn.sigmoid(pre_gate)
    silu_gate = pre_gate * sig_gate
    act_b = (silu_gate * pre_up).astype(jnp.bfloat16)
    g_bf = g_acc.astype(jnp.bfloat16)
    d_act = jnp.dot(g_bf, down_w.T, preferred_element_type=jnp.float32)
    grad_down = jnp.dot(act_b.T, g_bf, preferred_element_type=jnp.float32)
    d_gate_b = (d_act * pre_up * sig_gate * (1.0 + pre_gate * (1.0 - sig_gate))).astype(jnp.bfloat16)
    d_up_b = (d_act * silu_gate).astype(jnp.bfloat16)
    grad_gate = jnp.dot(norm_b.T, d_gate_b, preferred_element_type=jnp.float32)
    grad_up = jnp.dot(norm_b.T, d_up_b, preferred_element_type=jnp.float32)
    d_norm = jnp.dot(d_gate_b, gate_w.T, preferred_element_type=jnp.float32) + jnp.dot(d_up_b, up_w.T, preferred_element_type=jnp.float32)
    d_x = inv_rms * (d_norm - norm_f * jnp.mean(d_norm * norm_f, axis=-1, keepdims=True))
    return g_acc + d_x, grad_gate, grad_up, grad_down


def reference(h_saved, grad_out, w_gate, w_up, w_down):
    h_blocks = h_saved.reshape(LAYERS, SHARDS, TOK_SHARD, D)
    g_init = grad_out.reshape(SHARDS, TOK_SHARD, D).astype(jnp.float32)

    def layer_step(g_all, layer_in):
        h_layer, gate_w, up_w, down_w = layer_in
        zero_in = jnp.zeros((D, FF), jnp.float32)
        zero_out = jnp.zeros((FF, D), jnp.float32)

        def shard_step(sums, shard_in):
            h_in, g_acc = shard_in
            g_next, grad_gate, grad_up, grad_down = layer_backward(h_in, g_acc, gate_w, up_w, down_w)
            return (sums[0] + grad_gate, sums[1] + grad_up, sums[2] + grad_down), g_next

        sums, g_new = lax.scan(shard_step, (zero_in, zero_in, zero_out), (h_layer, g_all))
        return g_new, sums

    g_final, grads = lax.scan(layer_step, g_init, (h_blocks, w_gate, w_up, w_down), reverse=True)
    d_h0 = g_final.reshape(BATCH, SEQ, D).astype(jnp.bfloat16)
    return grads[0], grads[1], grads[2], d_h0
```

```python
import functools

import jax
import jax.numpy as jnp
from jax import lax
from jax.experimental import pallas as pl
from jax.experimental.pallas import tpu as pltpu
from jax.sharding import PartitionSpec as P

EPS = 1e-5
MESH = pl.DeviceIdType.MESH
F32 = jnp.float32
BF16 = jnp.bfloat16
FB = 256
LEAD = 8
BASE = 240
DOT_NT = (((1,), (1,)), ((), ()))


def ring(i, n):
    return lax.rem(i + BASE, n)


def dot(a, b):
    return jnp.dot(a, b, preferred_element_type=F32)


def dot_nt(a, b):
    return lax.dot_general(a, b, DOT_NT, preferred_element_type=F32)


def kernel(
    dims, h_ref, g_ref, wgu_ref, wd_ref,
    dg_ref, du_ref, dd_ref, dh_ref, ggu, gwd, gt_ref,
    n_t, gb_t, dn_t, r_row, wgu_b, wd_b, w_t, s_a, s_du, s_dv, acc, hb,
    sg, sd, rdg, rdd, xsg, xsd, pog, pod, rxg, rxd, ysg, ysd, ryg, ryd, fog, fod,
    wl_sem, d_snd, d_rcv, x_snd, x_rcv, y_snd, y_rcv, o_sem, f_loc, f_snd, f_rcv,
    w_snd, w_rcv, hb_sem, gl_sem, gs_sem, do_sem,
):
    layers, tokens, width, hidden, tb, nb = dims
    dq = width // 4
    hq = dq // 2
    half = hidden // 2
    nj = hidden // FB
    mid = nj // 2
    steps = layers * nj
    y = lax.axis_index("dp")
    me = lax.axis_index("fsdp")
    x = me // 2
    c = me % 2
    qx = (1 - x) * 2 + c
    partner = (y, x * 2 + 1 - c)
    x_dev = (y, qx)
    y_dev = (1 - y, me)

    def layer_of(s):
        return layers - 1 - s // nj

    def block_of(t):
        return t // 2 + (t % 2) * (mid + 1)

    def owner_piece(t, e):
        last = t // (nj - 1)
        core = (1 - last) * (t % 2) + last * e
        piece = (1 - last) * (t + e) + last * (nj - 1) * (1 - e)
        return core, piece

    def remote(src, dst, snd, rcv, dev):
        return pltpu.make_async_remote_copy(
            src_ref=src, dst_ref=dst, send_sem=snd, recv_sem=rcv, device_id=dev, device_id_type=MESH
        )

    def weight_copies(kind, p):
        l, t = layer_of(p), p % nj
        rs = ring(p, 8)
        if kind in "AB":
            gu_src, wd_src, q = wgu_ref.at[l, block_of(t)], wd_ref.at[l, t], me
        else:
            gu_src, wd_src, q = ggu.at[p, qx], gwd.at[p, qx], qx
        gu_dst, wd_dst = ggu.at[p, q], gwd.at[p, q]
        if kind != "A":
            side = 1 - y if kind == "E" else y
            rows = pl.ds(pl.multiple_of(side * hq, 16), hq)
            rows_d = pl.ds(pl.multiple_of(side * 32, 32), 32)
            gu_src, gu_dst = gu_src.at[:, rows], gu_dst.at[:, rows]
            wd_src, wd_dst = wd_src.at[rows_d], wd_dst.at[rows_d]
        dev = {"A": partner, "B": x_dev, "C": y_dev, "D": partner, "E": partner}[kind]
        k = "ABCDE".index(kind)
        return (
            remote(gu_src, gu_dst, w_snd.at[k, 0, rs], w_rcv.at[k, 0, rs], dev),
            remote(wd_src, wd_dst, w_snd.at[k, 1, rs], w_rcv.at[k, 1, rs], dev),
        )

    def weight_start(kinds, p):
        @pl.when((p >= 0) & (p < steps))
        def _():
            for kind in kinds:
                for cp in weight_copies(kind, p):
                    cp.start()

    def weight_wait_recv(kinds, p):
        @pl.when((p >= 0) & (p < steps))
        def _():
            for kind in kinds:
                for cp in weight_copies(kind, p):
                    cp.wait_recv()

    def weight_wait_send(kinds, p):
        @pl.when((p >= 0) & (p < steps))
        def _():
            for kind in kinds:
                for cp in weight_copies(kind, p):
                    cp.wait_send()

    def load_weights(s, go):
        slot = ring(s, 2)
        l, t = layer_of(s), s % nj

        def act(src, dst, i):
            cp = pltpu.make_async_copy(src, dst, wl_sem.at[slot, i])
            cp.start() if go else cp.wait()

        for d in range(4):
            q = (me + d) % 4
            dst = wgu_b.at[slot, :, pl.ds(pl.multiple_of(q * dq, 16), dq)]
            act(wgu_ref.at[l, block_of(t)] if d == 0 else ggu.at[s, q], dst, d)
        for e in range(2):
            core, piece = owner_piece(t, e)
            for xx in range(2):
                q = xx * 2 + core
                dst = wd_b.at[slot, pl.ds(xx * 128 + e * 64, 64)]
                i = 4 + e * 2 + xx
                if go:
                    @pl.when(q == me)
                    def _():
                        act(wd_ref.at[l, piece], dst, i)

                    @pl.when(q != me)
                    def _():
                        act(gwd.at[s - t + piece, q], dst, i)
                else:
                    act(wd_ref.at[l, piece], dst, i)

    def core_copies(b):
        r, a, z = ring(b, 8), ring(b, 2), ring(b, 3)
        return (
            remote(sg.at[a, :, :, 1 - c], rdg.at[z], d_snd.at[0, r], d_rcv.at[0, r], partner),
            remote(sd.at[a, :, 1 - c], rdd.at[z], d_snd.at[1, r], d_rcv.at[1, r], partner),
        )

    def x_copies(b):
        r, a, z = ring(b, 8), ring(b, 3), ring(b, 5)
        return (
            remote(xsg.at[a], rxg.at[z], x_snd.at[0, r], x_rcv.at[0, r], x_dev),
            remote(xsd.at[a], rxd.at[z], x_snd.at[1, r], x_rcv.at[1, r], x_dev),
        )

    def y_copies(b):
        r, a, z = ring(b, 8), ring(b, 3), ring(b, 5)
        return (
            remote(ysg.at[a], ryg.at[z], y_snd.at[0, r], y_rcv.at[0, r], y_dev),
            remote(ysd.at[a], ryd.at[z], y_snd.at[1, r], y_rcv.at[1, r], y_dev),
        )

    def valid(b):
        return (b >= 0) & (b < steps)

    def start_all(copies, b):
        @pl.when(valid(b))
        def _():
            for cp in copies(b):
                cp.start()

    def wait_all(copies, b):
        @pl.when(valid(b))
        def _():
            for cp in copies(b):
                cp.wait_recv()
            for cp in copies(b):
                cp.wait_send()

    def out_gate_up(b):
        a = ring(b, 2)
        l, m = layer_of(b), block_of(b % nj)
        cps = []
        for gu, out in enumerate((dg_ref, du_ref)):
            for hf in range(2):
                cols = pl.ds(pl.multiple_of(hf * half + m * 128, 128), 128)
                src = fog.at[a, gu, :, pl.ds(hf * 128, 128)]
                cps.append(pltpu.make_async_copy(src, out.at[l, :, cols], o_sem.at[gu * 2 + hf, a]))
        return cps

    def out_down(b, own):
        a, r = ring(b, 2), ring(b, 4)
        core, piece = owner_piece(b % nj, c)
        dst = dd_ref.at[layer_of(b), pl.ds(pl.multiple_of(piece * 64, 64), 64)]
        if own:
            return pltpu.make_async_copy(fod.at[a], dst, f_loc.at[a])
        return remote(fod.at[a], dst, f_snd.at[r], f_rcv.at[r], partner)

    def out_start(b):
        @pl.when(valid(b))
        def _():
            for cp in out_gate_up(b):
                cp.start()
            core, _ = owner_piece(b % nj, c)

            @pl.when(core == c)
            def _():
                out_down(b, True).start()

            @pl.when(core != c)
            def _():
                out_down(b, False).start()

    def out_wait(b):
        @pl.when(valid(b))
        def _():
            for cp in out_gate_up(b):
                cp.wait()
            core, _ = owner_piece(b % nj, c)
            theirs, _ = owner_piece(b % nj, 1 - c)

            @pl.when(core == c)
            def _():
                out_down(b, True).wait()

            @pl.when(core != c)
            def _():
                out_down(b, False).wait_send()

            @pl.when(theirs == c)
            def _():
                out_down(b, False).wait_recv()

    def boundary(s):
        @pl.when((s >= 0) & (s < steps))
        def _():
            load_weights(s, False)

        wait_all(core_copies, s - 2)
        wait_all(x_copies, s - 5)
        wait_all(y_copies, s - 8)
        out_wait(s - 10)
        p = s + LEAD
        weight_wait_recv("B", p - 2)
        weight_wait_recv("C", p - 4)
        weight_wait_recv("ADE", p - 6)
        weight_wait_send("AB", p - 2)
        weight_wait_send("CD", p - 4)
        weight_wait_send("E", p - 6)
        weight_start("B", p)
        weight_start("A", p)
        weight_start("CD", p - 2)
        weight_start("E", p - 4)
        start_all(core_copies, s - 1)
        start_all(x_copies, s - 3)
        start_all(y_copies, s - 6)
        out_start(s - 9)

        @pl.when((s + 1 >= 0) & (s + 1 < steps))
        def _():
            load_weights(s + 1, True)

    def sums(s):
        a, b5, b3 = ring(s - 8, 2), ring(s - 8, 5), ring(s - 8, 3)
        for i in range(2):
            fog[a, i] = ysg[b3, i] + ryg[b5, i]
        fod[a] = ysd[b3] + ryd[b5]
        a, b5 = ring(s - 5, 3), ring(s - 5, 5)
        for i in range(2):
            ysg[a, i] = pog[a, i] + rxg[b5, i]
        ysd[a] = pod[a] + rxd[b5]
        a, b3 = ring(s - 2, 2), ring(s - 2, 3)
        for i in range(2):
            pog[b3, i] = sg[a, i, x, c] + rdg[b3, i, x]
            xsg[b3, i] = sg[a, i, 1 - x, c] + rdg[b3, i, 1 - x]
        pod[b3] = sd[a, x, c] + rdd[b3, x]
        xsd[b3] = sd[a, 1 - x, c] + rdd[b3, 1 - x]

    def compute(s):
        slot = ring(s, 2)
        for i in range(2):
            w_t[i] = wgu_b[slot, i].T
        blocks = tokens // tb

        def first(t):
            tok = pl.ds(t * tb, tb)
            u = dot(w_t[0], n_t[:, tok])
            v = dot(w_t[1], n_t[:, tok])
            da = dot(wd_b[slot], gb_t[:, tok])
            sig = jax.nn.sigmoid(u)
            silu = u * sig
            s_a[t % 2] = (silu * v).astype(BF16)
            s_du[t % 2] = (da * v * sig * (1.0 + u * (1.0 - sig))).astype(BF16)
            s_dv[t % 2] = (da * silu).astype(BF16)

        def second(t):
            tok = pl.ds(t * tb, tb)
            for i, val in enumerate((s_du, s_dv)):
                part = dot_nt(n_t[:, tok], val[t % 2])
                if t > 0:
                    part = acc[i] + part
                if t < blocks - 1:
                    acc[i] = part
                else:
                    sg[slot, i] = part.reshape(2, 2, dq, FB)
            part = dot_nt(gb_t[:, tok], s_a[t % 2])
            if t > 0:
                part = acc[2] + part
            if t < blocks - 1:
                acc[2] = part
            else:
                sd[slot] = part.T.reshape(2, 2, 64, width)
            dn_t[:, tok] += dot(wgu_b[slot, 0], s_du[t % 2]) + dot(wgu_b[slot, 1], s_dv[t % 2])

        first(0)
        for t in range(1, blocks):
            first(t)
            second(t - 1)
        second(blocks - 1)

    n_tok = tokens // nb

    def tok_of(i):
        return pl.ds(pl.multiple_of(i * nb, nb), nb)

    def rows_load(i, src, which):
        return pltpu.make_async_copy(src.at[tok_of(i)], hb.at[ring(i, 2), which], hb_sem.at[ring(i, 2), which])

    def g_load(i):
        return pltpu.make_async_copy(gt_ref.at[:, tok_of(i)], acc.at[ring(i, 3)], gl_sem.at[ring(i, 3)])

    def g_store(i):
        return pltpu.make_async_copy(acc.at[ring(i, 3)], gt_ref.at[:, tok_of(i)], gs_sem.at[ring(i, 3)])

    groups = [pl.ds(k, 128) for k in range(0, width, 128)]

    def new_norm(i):
        tok = tok_of(i)
        total = jnp.zeros((1, nb), F32)
        for rows in groups:
            xt = hb[ring(i, 2), 1, :, rows].T
            n_t[rows, tok] = xt
            xf = xt.astype(F32)
            total += jnp.sum(xf * xf, axis=0, keepdims=True)
        r = lax.rsqrt(total * (1.0 / width) + EPS)
        r_row[:, tok] = r
        for rows in groups:
            n_t[rows, tok] = (n_t[rows, tok].astype(F32) * r).astype(BF16)
            dn_t[rows, tok] = jnp.zeros((128, nb), F32)

    def new_g(i, put):
        tok = tok_of(i)
        r = r_row[:, tok]
        total = jnp.zeros((1, nb), F32)
        for rows in groups:
            xt = hb[ring(i, 2), 0, :, rows].T
            gb_t[rows, tok] = xt
            total += jnp.sum(dn_t[rows, tok] * (xt.astype(F32) * r), axis=0, keepdims=True)
        m = total * (1.0 / width)
        for rows in groups:
            nf = gb_t[rows, tok].astype(F32) * r
            put(rows, acc[ring(i, 3), rows] + r * (dn_t[rows, tok] - nf * m))

    def enter_block(i):
        h_new = h_ref.at[layers - 1]

        @pl.when(i == 0)
        def _():
            rows_load(i, g_ref, 0).start()
            rows_load(i, h_new, 1).start()

        @pl.when(i + 1 < n_tok)
        def _():
            rows_load(i + 1, g_ref, 0).start()
            rows_load(i + 1, h_new, 1).start()

        @pl.when(i >= 3)
        def _():
            g_store(i - 3).wait()

        rows_load(i, g_ref, 0).wait()
        rows_load(i, h_new, 1).wait()
        for rows in groups:
            gb = hb[ring(i, 2), 0, :, rows].T
            gb_t[rows, tok_of(i)] = gb
            acc[ring(i, 3), rows] = gb.astype(F32)
        new_norm(i)
        g_store(i).start()

    def stores_done():
        for i in range(n_tok - 3, n_tok):
            g_store(i).wait()

    def between(l_new):
        h_old, h_new = h_ref.at[l_new + 1], h_ref.at[l_new]
        rows_load(0, h_old, 0).start()
        rows_load(0, h_new, 1).start()
        g_load(0).start()

        def body(i, _):
            @pl.when(i >= 2)
            def _():
                g_store(i - 2).wait()

            @pl.when(i + 1 < n_tok)
            def _():
                rows_load(i + 1, h_old, 0).start()
                rows_load(i + 1, h_new, 1).start()
                g_load(i + 1).start()

            rows_load(i, h_old, 0).wait()
            rows_load(i, h_new, 1).wait()
            g_load(i).wait()

            def put(rows, g):
                acc[ring(i, 3), rows] = g
                gb_t[rows, tok_of(i)] = g.astype(BF16)

            new_g(i, put)
            new_norm(i)
            g_store(i).start()
            return 0

        lax.fori_loop(0, n_tok, body, 0)
        for i in range(n_tok - 2, n_tok):
            g_store(i).wait()

    def leave():
        h_old = h_ref.at[0]

        def dh_store(i):
            return pltpu.make_async_copy(hb.at[ring(i, 2), 1], dh_ref.at[tok_of(i)], do_sem.at[ring(i, 2)])

        rows_load(0, h_old, 0).start()
        g_load(0).start()

        def body(i, _):
            @pl.when(i + 1 < n_tok)
            def _():
                rows_load(i + 1, h_old, 0).start()
                g_load(i + 1).start()

            @pl.when(i >= 2)
            def _():
                dh_store(i - 2).wait()

            rows_load(i, h_old, 0).wait()
            g_load(i).wait()

            def put(rows, g):
                hb[ring(i, 2), 1, :, rows] = g.astype(BF16).T

            new_g(i, put)
            dh_store(i).start()
            return 0

        lax.fori_loop(0, n_tok, body, 0)
        for i in range(n_tok - 2, n_tok):
            dh_store(i).wait()

    barrier = pltpu.get_barrier_semaphore()
    for dev in (partner, x_dev, y_dev):
        pl.semaphore_signal(barrier, inc=1, device_id=dev, device_id_type=MESH)
    pl.semaphore_wait(barrier, 3)

    per = n_tok // LEAD

    def lead_in(i, _):
        boundary(i - LEAD)
        for k in range(per):
            enter_block(i * per + k)
        return 0

    lax.fori_loop(0, LEAD, lead_in, 0)
    stores_done()

    def main(s, _):
        boundary(s)

        @pl.when((s % nj == 0) & (s > 0))
        def _():
            between(layer_of(s))

        sums(s)
        compute(s)
        return 0

    lax.fori_loop(0, steps, main, 0)
    boundary(steps)
    sums(steps)
    leave()

    def drain(s, _):
        boundary(s)
        sums(s)
        return 0

    lax.fori_loop(steps + 1, steps + 10, drain, 0)


def backward(dims, h, g, wgu, wd):
    layers, tokens, width, hidden, tb, nb = dims
    dq = width // 4
    nj = hidden // FB
    steps = layers * nj
    dma = pltpu.SemaphoreType.DMA
    vm = pltpu.VMEM
    anyspace = pl.BlockSpec(memory_space=pl.ANY)
    sds = jax.ShapeDtypeStruct
    out_shape = [
        sds((layers, dq, hidden), F32),
        sds((layers, dq, hidden), F32),
        sds((layers, hidden // 4, width), F32),
        sds((tokens, width), BF16),
        sds((steps, 4, 2, dq, FB), BF16),
        sds((steps, 4, 64, width), BF16),
        sds((width, tokens), F32),
    ]

    def pair(n):
        return [vm((n, 2, dq, FB), F32), vm((n, 64, width), F32)]

    scratch = [
        vm((width, tokens), BF16),
        vm((width, tokens), BF16),
        vm((width, tokens), F32),
        vm((1, tokens), F32),
        vm((2, 2, width, FB), BF16),
        vm((2, FB, width), BF16),
        vm((2, FB, width), BF16),
        vm((2, FB, tb), BF16),
        vm((2, FB, tb), BF16),
        vm((2, FB, tb), BF16),
        vm((3, width, FB), F32),
        vm((2, 2, nb, width), BF16),
        vm((2, 2, 2, 2, dq, FB), F32),
        vm((2, 2, 2, 64, width), F32),
        vm((3, 2, 2, dq, FB), F32),
        vm((3, 2, 64, width), F32),
        *pair(3), *pair(3), *pair(5), *pair(3), *pair(5), *pair(2),
        dma((2, 8)),
        dma((2, 8)), dma((2, 8)), dma((2, 8)), dma((2, 8)), dma((2, 8)), dma((2, 8)),
        dma((4, 2)), dma((2,)), dma((4,)), dma((4,)),
        dma((5, 2, 8)), dma((5, 2, 8)),
        dma((2, 2)), dma((3,)), dma((3,)), dma((2,)),
    ]
    return pl.pallas_call(
        functools.partial(kernel, dims),
        out_shape=out_shape,
        in_specs=[anyspace] * 4,
        out_specs=[anyspace] * 7,
        scratch_shapes=scratch,
        compiler_params=pltpu.CompilerParams(
            collective_id=0, has_side_effects=True, vmem_limit_bytes=67043328
        ),
        name="mlp_backward",
    )(h, g, wgu, wd)[:4]


def solution(mesh):
    tok_spec = P(("dp", "fsdp"))
    stack_spec = P(None, ("dp", "fsdp"))
    weight_spec = P(None, "fsdp")

    def local_backward(h_saved, grad_out, gate_sh, up_sh, down_sh):
        layers = h_saved.shape[0]
        b_loc, seq, width = grad_out.shape
        tokens = b_loc * seq
        dq, hidden = gate_sh.shape[1:]
        nj = hidden // FB
        tb = min(256, tokens // 2)
        nb = FB
        wgu = jnp.stack([gate_sh, up_sh], axis=1).reshape(layers, 2, dq, 2, nj, 128)
        wgu = wgu.transpose(0, 4, 1, 2, 3, 5).reshape(layers, nj, 2, dq, FB)
        wd = down_sh.reshape(layers, nj, 64, width)
        dims = (layers, tokens, width, hidden, tb, nb)
        d_gate, d_up, d_down, d_h0 = backward(
            dims, h_saved.reshape(layers, tokens, width), grad_out.reshape(tokens, width), wgu, wd
        )
        return d_gate, d_up, d_down, d_h0.reshape(b_loc, seq, width)

    return jax.shard_map(
        local_backward,
        mesh=mesh,
        in_specs=(stack_spec, tok_spec, weight_spec, weight_spec, weight_spec),
        out_specs=(weight_spec, weight_spec, weight_spec, tok_spec),
        check_vma=False,
    )
```

```python
import functools

import jax
import jax.numpy as jnp
from jax import lax
from jax.experimental import pallas as pl
from jax.experimental.pallas import tpu as pltpu
from jax.sharding import PartitionSpec as P

EPS = 1e-5
MESH = pl.DeviceIdType.MESH
F32 = jnp.float32
BF16 = jnp.bfloat16
FB = 256
LEAD = 8
BURST = 6
RS = 32
BASE = 240
DOT_NT = (((1,), (1,)), ((), ()))


def div(a, b):
    return a // b if isinstance(a, int) else lax.div(a, jnp.int32(b))


def rem(a, b):
    return a % b if isinstance(a, int) else lax.rem(a, jnp.int32(b))


def ring(i, n):
    return rem(i + BASE, n)


def dot(a, b):
    return jnp.dot(a, b, preferred_element_type=F32)


def dot_nt(a, b):
    return lax.dot_general(a, b, DOT_NT, preferred_element_type=F32)


def kernel(
    dims, h_ref, g_ref, gate_ref, up_ref, wd_ref,
    dg_ref, du_ref, dd_ref, dh_ref, ggu, gwd, gt_ref,
    n_t, gb_t, dn_t, r_row, wgu_b, wd_b, s_a, s_du, s_dv, acc, hb,
    sg, sd, rdg, rdd, xsg, xsd, pog, pod, rxg, rxd, ysg, ysd, ryg, ryd, fog, fod,
    wl_sem, d_snd, d_rcv, x_snd, x_rcv, y_snd, y_rcv, o_sem, f_loc, f_snd, f_rcv,
    w_snd, w_rcv, hb_sem, gl_sem, gs_sem, do_sem,
):
    layers, tokens, width, hidden, tb, sub, nb = dims
    dq = width // 4
    hq = dq // 2
    half = hidden // 2
    nj = hidden // FB
    mid = nj // 2
    steps = layers * nj
    y = lax.axis_index("dp")
    me = lax.axis_index("fsdp")
    x = me // 2
    c = me % 2
    qx = (1 - x) * 2 + c
    partner = (y, x * 2 + 1 - c)
    x_dev = (y, qx)
    y_dev = (1 - y, me)

    def layer_of(s):
        return layers - 1 - div(s, nj)

    def block_of(t):
        return div(t, 2) + rem(t, 2) * (mid + 1)

    def owner_piece(t, e):
        last = div(t, nj - 1)
        core = (1 - last) * rem(t, 2) + last * e
        piece = (1 - last) * (t + e) + last * (nj - 1) * (1 - e)
        return core, piece

    def remote(src, dst, snd, rcv, dev):
        return pltpu.make_async_remote_copy(
            src_ref=src, dst_ref=dst, send_sem=snd, recv_sem=rcv, device_id=dev, device_id_type=MESH
        )

    def next_piece(beta, n):
        burst = ((beta >= LEAD) & (beta < LEAD + 3)).astype(jnp.int32)
        skip = ((beta >= LEAD + 3) & (rem(beta, 6) == 4)).astype(jnp.int32)
        return n + (1 + (BURST - 1) * burst - skip) * (n < steps).astype(jnp.int32)

    def shard_parts(l, t, rows):
        m = block_of(t)
        for gu, ref in enumerate((gate_ref, up_ref)):
            for hf in range(2):
                cols = pl.ds(pl.multiple_of(hf * half + m * 128, 128), 128)
                yield ref.at[l, rows, cols], gu, pl.ds(hf * 128, 128)

    def weight_copies(kind, p, whole):
        l, t = layer_of(p), rem(p, nj)
        rs = ring(p, RS)
        k = "ABCDE".index(kind)
        q = me if kind in "AB" else qx
        dev = {"A": partner, "B": x_dev, "C": y_dev, "D": partner, "E": partner}[kind]
        if kind == "A":
            rows, rows_d = pl.ds(0, dq), pl.ds(0, 64)
        else:
            side = 1 - y if kind == "E" else y
            rows = pl.ds(pl.multiple_of(side * hq, 16), hq)
            rows_d = pl.ds(pl.multiple_of(side * 32, 32), 32)
        sems = w_snd.at[k, 0, rs], w_rcv.at[k, 0, rs]
        if kind in "AB" and not whole:
            for src, gu, lanes in shard_parts(l, t, rows):
                yield remote(src, ggu.at[p, q, gu, rows, lanes], *sems, dev)
        else:
            both = ggu.at[p, q, :, rows]
            yield remote(both, both, *sems, dev)
        wd_dst = gwd.at[p, q, rows_d]
        wd_src = wd_ref.at[l, t, rows_d] if kind in "AB" else wd_dst
        yield remote(wd_src, wd_dst, w_snd.at[k, 1, rs], w_rcv.at[k, 1, rs], dev)

    def pieces(span, act):
        def body(p, _):
            act(p)
            return 0

        lax.fori_loop(*span, body, 0)

    def weight_start(kinds, p):
        for kind in kinds:
            for cp in weight_copies(kind, p, False):
                cp.start()

    def weight_wait_recv(kinds, p):
        for kind in kinds:
            for cp in weight_copies(kind, p, True):
                cp.wait_recv()

    def weight_wait_send(kinds, p):
        for kind in kinds:
            for cp in weight_copies(kind, p, True):
                cp.wait_send()

    def weights_wait(sent):
        def arrived_x(p):
            weight_wait_recv("B", p)
            weight_wait_send("AB", p)

        def arrived_y(p):
            weight_wait_recv("C", p)
            weight_wait_send("CD", p)

        def complete(p):
            weight_wait_recv("ADE", p)
            weight_wait_send("E", p)

        pieces((sent[3], sent[2]), arrived_x)
        pieces((sent[5], sent[4]), arrived_y)
        pieces((sent[7], sent[6]), complete)

    def weights_send(sent):
        pieces((sent[1], sent[0]), functools.partial(weight_start, "BA"))
        pieces((sent[3], sent[2]), functools.partial(weight_start, "CD"))
        pieces((sent[5], sent[4]), functools.partial(weight_start, "E"))

    def load_weights(s, go):
        slot = ring(s, 2)
        l, t = layer_of(s), rem(s, nj)

        def act(src, dst, i):
            cp = pltpu.make_async_copy(src, dst, wl_sem.at[slot, i])
            cp.start() if go else cp.wait()

        for d in range(4):
            q = rem(me + d, 4)
            rows = pl.ds(pl.multiple_of(q * dq, 16), dq)
            if d == 0 and go:
                for src, gu, lanes in shard_parts(l, t, pl.ds(0, dq)):
                    act(src, wgu_b.at[slot, gu, rows, lanes], d)
            else:
                act(ggu.at[s, q], wgu_b.at[slot, :, rows], d)
        for e in range(2):
            core, piece = owner_piece(t, e)
            for xx in range(2):
                q = xx * 2 + core
                dst = wd_b.at[slot, pl.ds(xx * 128 + e * 64, 64)]
                i = 4 + e * 2 + xx
                if go:
                    @pl.when(q == me)
                    def _():
                        act(wd_ref.at[l, piece], dst, i)

                    @pl.when(q != me)
                    def _():
                        act(gwd.at[s - t + piece, q], dst, i)
                else:
                    act(wd_ref.at[l, piece], dst, i)

    def core_copies(b):
        r, a, z = ring(b, 8), ring(b, 2), ring(b, 2)
        return (
            remote(sg.at[a, :, :, 1 - c], rdg.at[z], d_snd.at[0, r], d_rcv.at[0, r], partner),
            remote(sd.at[a, :, 1 - c], rdd.at[z], d_snd.at[1, r], d_rcv.at[1, r], partner),
        )

    def x_copies(b):
        r, a, z = ring(b, 8), ring(b, 2), ring(b, 4)
        return (
            remote(xsg.at[a], rxg.at[z], x_snd.at[0, r], x_rcv.at[0, r], x_dev),
            remote(xsd.at[a], rxd.at[z], x_snd.at[1, r], x_rcv.at[1, r], x_dev),
        )

    def y_copies(b):
        r, a, z = ring(b, 8), ring(b, 2), ring(b, 4)
        return (
            remote(ysg.at[a], ryg.at[z], y_snd.at[0, r], y_rcv.at[0, r], y_dev),
            remote(ysd.at[a], ryd.at[z], y_snd.at[1, r], y_rcv.at[1, r], y_dev),
        )

    def valid(b):
        return (b >= 0) & (b < steps)

    def start_all(copies, b):
        @pl.when(valid(b))
        def _():
            for cp in copies(b):
                cp.start()

    def wait_all(copies, b):
        @pl.when(valid(b))
        def _():
            for cp in copies(b):
                cp.wait_recv()
            for cp in copies(b):
                cp.wait_send()

    def out_gate_up(b):
        a = ring(b, 2)
        l, m = layer_of(b), block_of(rem(b, nj))
        cps = []
        for gu, out in enumerate((dg_ref, du_ref)):
            for hf in range(2):
                cols = pl.ds(pl.multiple_of(hf * half + m * 128, 128), 128)
                src = fog.at[a, gu, :, pl.ds(hf * 128, 128)]
                cps.append(pltpu.make_async_copy(src, out.at[l, :, cols], o_sem.at[gu * 2 + hf, a]))
        return cps

    def out_down(b, own):
        a, r = ring(b, 2), ring(b, 8)
        core, piece = owner_piece(rem(b, nj), c)
        dst = dd_ref.at[layer_of(b), pl.ds(pl.multiple_of(piece * 64, 64), 64)]
        if own:
            return pltpu.make_async_copy(fod.at[a], dst, f_loc.at[a])
        return remote(fod.at[a], dst, f_snd.at[r], f_rcv.at[r], partner)

    def out_start(b):
        @pl.when(valid(b))
        def _():
            for cp in out_gate_up(b):
                cp.start()
            core, _ = owner_piece(rem(b, nj), c)

            @pl.when(core == c)
            def _():
                out_down(b, True).start()

            @pl.when(core != c)
            def _():
                out_down(b, False).start()

    def out_wait(b):
        @pl.when(valid(b))
        def _():
            for cp in out_gate_up(b):
                cp.wait()
            core, _ = owner_piece(rem(b, nj), c)
            theirs, _ = owner_piece(rem(b, nj), 1 - c)

            @pl.when(core == c)
            def _():
                out_down(b, True).wait()

            @pl.when(core != c)
            def _():
                out_down(b, False).wait_send()

            @pl.when(theirs == c)
            def _():
                out_down(b, False).wait_recv()

    def sum_y(b):
        a, z = ring(b, 2), ring(b, 4)
        for i in range(2):
            fog[a, i] = ysg[a, i] + ryg[z, i]
        fod[a] = ysd[a] + ryd[z]

    def sum_x(b):
        a, z = ring(b, 2), ring(b, 4)
        for i in range(2):
            ysg[a, i] = pog[a, i] + rxg[z, i]
        ysd[a] = pod[a] + rxd[z]

    def sum_cores(b):
        a = ring(b, 2)
        for i in range(2):
            pog[a, i] = sg[a, i, x, c] + rdg[a, i, x]
            xsg[a, i] = sg[a, i, 1 - x, c] + rdg[a, i, 1 - x]
        pod[a] = sd[a, x, c] + rdd[a, x]
        xsd[a] = sd[a, 1 - x, c] + rdd[a, 1 - x]

    def sums(s):
        @pl.when((s >= 6) & (s < steps + 2))
        def _():
            sum_y(s - 6)
            sum_x(s - 4)
            sum_cores(s - 2)

        for f, b, alone in ((sum_y, s - 6, s >= steps + 2), (sum_x, s - 4, (s < 6) | (s >= steps + 2)),
                            (sum_cores, s - 2, s < 6)):
            @pl.when(valid(b) & alone)
            def _():
                f(b)

    def boundary(s, sent):
        sent = (next_piece(s + LEAD, sent[0]), *sent[:-1])

        @pl.when((s >= 0) & (s < steps))
        def _():
            load_weights(s, False)

        wait_all(core_copies, s - 2)
        wait_all(x_copies, s - 4)
        wait_all(y_copies, s - 6)
        out_wait(s - 8)
        sums(s)
        weights_wait(sent)
        weights_send(sent)

        @pl.when((s + 1 >= 0) & (s + 1 < steps))
        def _():
            load_weights(s + 1, True)

        start_all(core_copies, s - 1)
        start_all(x_copies, s - 2)
        start_all(y_copies, s - 4)
        out_start(s - 6)
        return sent

    def compute(s):
        slot = ring(s, 2)
        for i in range(2):
            hb[0, i] = wgu_b[slot, i].T
        fine = tokens // tb
        coarse = fine // sub

        def first(t):
            tok = pl.ds(t * tb, tb)
            u = dot(hb[0, 0], n_t[:, tok])
            v = dot(hb[0, 1], n_t[:, tok])
            da = dot(wd_b[slot], gb_t[:, tok])
            sig = jax.nn.sigmoid(u)
            silu = u * sig
            at = (t // sub) % 2, slice(None), pl.ds((t % sub) * tb, tb)
            s_a[at] = (silu * v).astype(BF16)
            s_du[at] = (da * v * sig * (1.0 + u * (1.0 - sig))).astype(BF16)
            s_dv[at] = (da * silu).astype(BF16)

        def second(t):
            tok = pl.ds(t * tb * sub, tb * sub)
            for i, val in enumerate((s_du, s_dv)):
                part = dot_nt(n_t[:, tok], val[t % 2])
                if t > 0:
                    part = acc[i] + part
                if t < coarse - 1:
                    acc[i] = part
                else:
                    sg[slot, i] = part.reshape(2, 2, dq, FB)
            part = dot_nt(gb_t[:, tok], s_a[t % 2])
            if t > 0:
                part = acc[2] + part
            if t < coarse - 1:
                acc[2] = part
            else:
                sd[slot] = part.T.reshape(2, 2, 64, width)
            dn_t[:, tok] += dot(wgu_b[slot, 0], s_du[t % 2]) + dot(wgu_b[slot, 1], s_dv[t % 2])

        for t in range(coarse):
            for k in range(sub):
                first(t * sub + k)
            if t:
                second(t - 1)
        second(coarse - 1)

    n_tok = tokens // nb

    def tok_of(i):
        return pl.ds(pl.multiple_of(i * nb, nb), nb)

    def rows_load(i, src, which):
        return pltpu.make_async_copy(src.at[tok_of(i)], hb.at[ring(i, 2), which], hb_sem.at[ring(i, 2), which])

    def g_load(i):
        return pltpu.make_async_copy(gt_ref.at[:, tok_of(i)], acc.at[ring(i, 3)], gl_sem.at[ring(i, 3)])

    def g_store(i):
        return pltpu.make_async_copy(acc.at[ring(i, 3)], gt_ref.at[:, tok_of(i)], gs_sem.at[ring(i, 3)])

    groups = [pl.ds(k, 128) for k in range(0, width, 128)]

    def new_norm(i):
        tok = tok_of(i)
        total = jnp.zeros((1, nb), F32)
        for rows in groups:
            xt = hb[ring(i, 2), 1, :, rows].T
            n_t[rows, tok] = xt
            xf = xt.astype(F32)
            total += jnp.sum(xf * xf, axis=0, keepdims=True)
        r = lax.rsqrt(total * (1.0 / width) + EPS)
        r_row[:, tok] = r
        for rows in groups:
            n_t[rows, tok] = (n_t[rows, tok].astype(F32) * r).astype(BF16)
            dn_t[rows, tok] = jnp.zeros((128, nb), F32)

    def new_g(i, put):
        tok = tok_of(i)
        r = r_row[:, tok]
        total = jnp.zeros((1, nb), F32)
        for rows in groups:
            xt = hb[ring(i, 2), 0, :, rows].T
            gb_t[rows, tok] = xt
            total += jnp.sum(dn_t[rows, tok] * (xt.astype(F32) * r), axis=0, keepdims=True)
        m = total * (1.0 / width)
        for rows in groups:
            nf = gb_t[rows, tok].astype(F32) * r
            put(rows, acc[ring(i, 3), rows] + r * (dn_t[rows, tok] - nf * m))

    def enter_block(i):
        h_new = h_ref.at[layers - 1]

        @pl.when(i == 0)
        def _():
            rows_load(i, g_ref, 0).start()
            rows_load(i, h_new, 1).start()

        @pl.when(i + 1 < n_tok)
        def _():
            rows_load(i + 1, g_ref, 0).start()
            rows_load(i + 1, h_new, 1).start()

        @pl.when(i >= 3)
        def _():
            g_store(i - 3).wait()

        rows_load(i, g_ref, 0).wait()
        rows_load(i, h_new, 1).wait()
        for rows in groups:
            gb = hb[ring(i, 2), 0, :, rows].T
            gb_t[rows, tok_of(i)] = gb
            acc[ring(i, 3), rows] = gb.astype(F32)
        new_norm(i)
        g_store(i).start()

    def stores_done():
        for i in range(n_tok - 3, n_tok):
            g_store(i).wait()

    def between(l_new):
        h_old, h_new = h_ref.at[l_new + 1], h_ref.at[l_new]
        rows_load(0, h_old, 0).start()
        rows_load(0, h_new, 1).start()
        g_load(0).start()

        def body(i, _):
            @pl.when(i >= 2)
            def _():
                g_store(i - 2).wait()

            @pl.when(i + 1 < n_tok)
            def _():
                rows_load(i + 1, h_old, 0).start()
                rows_load(i + 1, h_new, 1).start()
                g_load(i + 1).start()

            rows_load(i, h_old, 0).wait()
            rows_load(i, h_new, 1).wait()
            g_load(i).wait()

            def put(rows, g):
                acc[ring(i, 3), rows] = g
                gb_t[rows, tok_of(i)] = g.astype(BF16)

            new_g(i, put)
            new_norm(i)
            g_store(i).start()
            return 0

        lax.fori_loop(0, n_tok, body, 0)
        for i in range(n_tok - 2, n_tok):
            g_store(i).wait()

    def leave():
        h_old = h_ref.at[0]

        def dh_store(i):
            return pltpu.make_async_copy(hb.at[ring(i, 2), 1], dh_ref.at[tok_of(i)], do_sem.at[ring(i, 2)])

        rows_load(0, h_old, 0).start()
        g_load(0).start()

        def body(i, _):
            @pl.when(i + 1 < n_tok)
            def _():
                rows_load(i + 1, h_old, 0).start()
                g_load(i + 1).start()

            @pl.when(i >= 2)
            def _():
                dh_store(i - 2).wait()

            rows_load(i, h_old, 0).wait()
            g_load(i).wait()

            def put(rows, g):
                hb[ring(i, 2), 1, :, rows] = g.astype(BF16).T

            new_g(i, put)
            dh_store(i).start()
            return 0

        lax.fori_loop(0, n_tok, body, 0)
        for i in range(n_tok - 2, n_tok):
            dh_store(i).wait()

    barrier = pltpu.get_barrier_semaphore()
    for dev in (partner, x_dev, y_dev):
        pl.semaphore_signal(barrier, inc=1, device_id=dev, device_id_type=MESH)
    pl.semaphore_wait(barrier, 3)

    per = n_tok // LEAD

    def lead_in(i, sent):
        sent = boundary(i - LEAD, sent)
        for k in range(per):
            enter_block(i * per + k)
        return sent

    sent = lax.fori_loop(0, LEAD, lead_in, (jnp.int32(0),) * 8)
    stores_done()

    def main(s, sent):
        sent = boundary(s, sent)

        @pl.when((rem(s, nj) == 0) & (s > 0))
        def _():
            between(layer_of(s))

        compute(s)
        return sent

    sent = lax.fori_loop(0, steps, main, sent)
    sent = boundary(jnp.int32(steps), sent)
    leave()
    lax.fori_loop(steps + 1, steps + 8, boundary, sent)


def backward(dims, h, g, gate, up, wd):
    layers, tokens, width, hidden, tb, sub, nb = dims
    dq = width // 4
    nj = hidden // FB
    steps = layers * nj
    dma = pltpu.SemaphoreType.DMA
    vm = pltpu.VMEM
    anyspace = pl.BlockSpec(memory_space=pl.ANY)
    sds = jax.ShapeDtypeStruct
    out_shape = [
        sds((layers, dq, hidden), F32),
        sds((layers, dq, hidden), F32),
        sds((layers, hidden // 4, width), F32),
        sds((tokens, width), BF16),
        sds((steps, 4, 2, dq, FB), BF16),
        sds((steps, 4, 64, width), BF16),
        sds((width, tokens), F32),
    ]

    def pair(n):
        return [vm((n, 2, dq, FB), F32), vm((n, 64, width), F32)]

    scratch = [
        vm((width, tokens), BF16),
        vm((width, tokens), BF16),
        vm((width, tokens), F32),
        vm((1, tokens), F32),
        vm((2, 2, width, FB), BF16),
        vm((2, FB, width), BF16),
        vm((2, FB, tb * sub), BF16),
        vm((2, FB, tb * sub), BF16),
        vm((2, FB, tb * sub), BF16),
        vm((3, width, FB), F32),
        vm((2, 2, nb, width), BF16),
        vm((2, 2, 2, 2, dq, FB), F32),
        vm((2, 2, 2, 64, width), F32),
        vm((2, 2, 2, dq, FB), F32),
        vm((2, 2, 64, width), F32),
        *pair(2), *pair(2), *pair(4), *pair(2), *pair(4), *pair(2),
        dma((2, 8)),
        dma((2, 8)), dma((2, 8)), dma((2, 8)), dma((2, 8)), dma((2, 8)), dma((2, 8)),
        dma((4, 2)), dma((2,)), dma((8,)), dma((8,)),
        dma((5, 2, RS)), dma((5, 2, RS)),
        dma((2, 2)), dma((3,)), dma((3,)), dma((2,)),
    ]
    return pl.pallas_call(
        functools.partial(kernel, dims),
        out_shape=out_shape,
        in_specs=[anyspace] * 5,
        out_specs=[anyspace] * 7,
        scratch_shapes=scratch,
        compiler_params=pltpu.CompilerParams(
            collective_id=0, has_side_effects=True, vmem_limit_bytes=67043328
        ),
        name="mlp_backward",
    )(h, g, gate, up, wd)[:4]


def solution(mesh):
    tok_spec = P(("dp", "fsdp"))
    stack_spec = P(None, ("dp", "fsdp"))
    weight_spec = P(None, "fsdp")

    def local_backward(h_saved, grad_out, gate_sh, up_sh, down_sh):
        layers = h_saved.shape[0]
        b_loc, seq, width = grad_out.shape
        tokens = b_loc * seq
        dq, hidden = gate_sh.shape[1:]
        nj = hidden // FB
        tb = min(512, tokens // 2)
        nb = FB
        wd = down_sh.reshape(layers, nj, 64, width)
        sub = 1
        dims = (layers, tokens, width, hidden, tb, sub, nb)
        d_gate, d_up, d_down, d_h0 = backward(
            dims, h_saved.reshape(layers, tokens, width), grad_out.reshape(tokens, width), gate_sh, up_sh, wd
        )
        return d_gate, d_up, d_down, d_h0.reshape(b_loc, seq, width)

    return jax.shard_map(
        local_backward,
        mesh=mesh,
        in_specs=(stack_spec, tok_spec, weight_spec, weight_spec, weight_spec),
        out_specs=(weight_spec, weight_spec, weight_spec, tok_spec),
        check_vma=False,
    )
```

```python
import functools

import jax
import jax.numpy as jnp
from jax import lax
from jax.experimental import pallas as pl
from jax.experimental.pallas import tpu as pltpu
from jax.sharding import PartitionSpec as P

EPS = 1e-5
MESH = pl.DeviceIdType.MESH
F32 = jnp.float32
BF16 = jnp.bfloat16
FB = 256
LEAD = 9
BURST = 6
RS = 32
SHORT = 6
BASE = 240
DOT_NT = (((1,), (1,)), ((), ()))


def div(a, b):
    return a // b if isinstance(a, int) else lax.div(a, jnp.int32(b))


def rem(a, b):
    return a % b if isinstance(a, int) else lax.rem(a, jnp.int32(b))


def ring(i, n):
    return rem(i + BASE, n)


def dot(a, b):
    return jnp.dot(a, b, preferred_element_type=F32)


def dot_nt(a, b):
    return lax.dot_general(a, b, DOT_NT, preferred_element_type=F32)


def kernel(
    dims, h_ref, g_ref, gate_ref, up_ref, wd_ref,
    dg_ref, du_ref, dd_ref, dh_ref, ggu, gwd, gt_ref,
    n_t, gb_t, dn_t, r_row, wgu_b, wd_b, s_a, s_du, s_dv, acc, hb,
    sg, sd, rdg, rdd, xsg, xsd, pog, pod, rxg, rxd, ysg, ysd, ryg, ryd, fog, fod,
    wl_sem, d_snd, d_rcv, x_snd, x_rcv, y_snd, y_rcv, o_sem, f_loc, f_snd, f_rcv,
    w_snd, w_rcv, hb_sem, gl_sem, gs_sem, do_sem,
):
    layers, tokens, width, hidden, tb, nb = dims
    dq = width // 4
    hq = dq // 2
    half = hidden // 2
    nj = hidden // FB
    mid = nj // 2
    steps = layers * nj
    y = lax.axis_index("dp")
    me = lax.axis_index("fsdp")
    x = me // 2
    c = me % 2
    qx = (1 - x) * 2 + c
    partner = (y, x * 2 + 1 - c)
    x_dev = (y, qx)
    y_dev = (1 - y, me)

    def layer_of(s):
        return layers - 1 - div(s, nj)

    def block_of(t):
        return div(t, 2) + rem(t, 2) * (mid + 1)

    def owner_piece(t, e):
        last = div(t, nj - 1)
        core = (1 - last) * rem(t, 2) + last * e
        piece = (1 - last) * (t + e) + last * (nj - 1) * (1 - e)
        return core, piece

    def remote(src, dst, snd, rcv, dev):
        return pltpu.make_async_remote_copy(
            src_ref=src, dst_ref=dst, send_sem=snd, recv_sem=rcv, device_id=dev, device_id_type=MESH
        )

    def next_piece(beta, n):
        burst = ((beta >= LEAD) & (beta < LEAD + 3)).astype(jnp.int32)
        skip = ((beta >= LEAD + 3) & (rem(beta, 5) == 4)).astype(jnp.int32)
        return n + (1 + (BURST - 1) * burst - skip) * (n < steps).astype(jnp.int32)

    def shard_parts(l, t, rows):
        m = block_of(t)
        for gu, ref in enumerate((gate_ref, up_ref)):
            for hf in range(2):
                cols = pl.ds(pl.multiple_of(hf * half + m * 128, 128), 128)
                yield ref.at[l, rows, cols], gu, pl.ds(hf * 128, 128)

    def weight_copies(kind, p, whole):
        l, t = layer_of(p), rem(p, nj)
        rs = ring(p, RS)
        k = "ABCDE".index(kind)
        q = me if kind in "AB" else qx
        dev = {"A": partner, "B": x_dev, "C": y_dev, "D": partner, "E": partner}[kind]
        if kind == "A":
            rows, rows_d = pl.ds(0, dq), pl.ds(0, 64)
        else:
            side = 1 - y if kind == "E" else y
            rows = pl.ds(pl.multiple_of(side * hq, 16), hq)
            rows_d = pl.ds(pl.multiple_of(side * 32, 32), 32)
        sems = w_snd.at[k, 0, rs], w_rcv.at[k, 0, rs]
        if kind in "AB" and not whole:
            for src, gu, lanes in shard_parts(l, t, rows):
                yield remote(src, ggu.at[p, q, gu, rows, lanes], *sems, dev)
        else:
            both = ggu.at[p, q, :, rows]
            yield remote(both, both, *sems, dev)
        wd_dst = gwd.at[p, q, rows_d]
        wd_src = wd_ref.at[l, t, rows_d] if kind in "AB" else wd_dst
        yield remote(wd_src, wd_dst, w_snd.at[k, 1, rs], w_rcv.at[k, 1, rs], dev)

    def pieces(span, act):
        def body(p, _):
            act(p)
            return 0

        lax.fori_loop(*span, body, 0)

    def weight_start(kinds, p):
        for kind in kinds:
            for cp in weight_copies(kind, p, False):
                cp.start()

    def weight_wait_recv(kinds, p):
        for kind in kinds:
            for cp in weight_copies(kind, p, True):
                cp.wait_recv()

    def weight_wait_send(kinds, p):
        for kind in kinds:
            for cp in weight_copies(kind, p, True):
                cp.wait_send()

    def weights_wait(sent):
        def arrived_x(p):
            weight_wait_recv("B", p)
            weight_wait_send("AB", p)

        def arrived_y(p):
            weight_wait_recv("C", p)
            weight_wait_send("CD", p)

        def complete(p):
            weight_wait_recv("ADE", p)
            weight_wait_send("E", p)

        pieces((sent[3], sent[2]), arrived_x)
        pieces((sent[5], sent[4]), arrived_y)
        pieces((sent[7], sent[6]), complete)

    def weights_send(sent):
        pieces((sent[1], sent[0]), functools.partial(weight_start, "BA"))
        pieces((sent[3], sent[2]), functools.partial(weight_start, "CD"))
        pieces((sent[5], sent[4]), functools.partial(weight_start, "E"))

    def load_weights(s, go):
        slot = ring(s, 3)
        l, t = layer_of(s), rem(s, nj)

        def act(src, dst, i):
            cp = pltpu.make_async_copy(src, dst, wl_sem.at[slot, i])
            cp.start() if go else cp.wait()

        for d in range(4):
            q = rem(me + d, 4)
            rows = pl.ds(pl.multiple_of(q * dq, 16), dq)
            if d == 0 and go:
                for src, gu, lanes in shard_parts(l, t, pl.ds(0, dq)):
                    act(src, wgu_b.at[slot, gu, rows, lanes], d)
            else:
                act(ggu.at[s, q], wgu_b.at[slot, :, rows], d)
        for e in range(2):
            core, piece = owner_piece(t, e)
            for xx in range(2):
                q = xx * 2 + core
                dst = wd_b.at[slot, pl.ds(xx * 128 + e * 64, 64)]
                i = 4 + e * 2 + xx
                if go:
                    @pl.when(q == me)
                    def _():
                        act(wd_ref.at[l, piece], dst, i)

                    @pl.when(q != me)
                    def _():
                        act(gwd.at[s - t + piece, q], dst, i)
                else:
                    act(wd_ref.at[l, piece], dst, i)

    def core_copies(b):
        r, a, z = ring(b, 8), ring(b, 2), ring(b, 2)
        return (
            remote(sg.at[a, :, :, 1 - c], rdg.at[z], d_snd.at[0, r], d_rcv.at[0, r], partner),
            remote(sd.at[a, :, 1 - c], rdd.at[z], d_snd.at[1, r], d_rcv.at[1, r], partner),
        )

    def x_copies(b):
        r, a, z = ring(b, 8), ring(b, 2), ring(b, 4)
        return (
            remote(xsg.at[a], rxg.at[z], x_snd.at[0, r], x_rcv.at[0, r], x_dev),
            remote(xsd.at[a], rxd.at[z], x_snd.at[1, r], x_rcv.at[1, r], x_dev),
        )

    def y_copies(b):
        r, a, z = ring(b, 8), ring(b, 2), ring(b, 4)
        return (
            remote(ysg.at[a], ryg.at[z], y_snd.at[0, r], y_rcv.at[0, r], y_dev),
            remote(ysd.at[a], ryd.at[z], y_snd.at[1, r], y_rcv.at[1, r], y_dev),
        )

    def valid(b):
        return (b >= 0) & (b < steps)

    def start_all(copies, b, cond=None):
        @pl.when(valid(b) if cond is None else valid(b) & cond)
        def _():
            for cp in copies(b):
                cp.start()

    def wait_all(copies, b):
        @pl.when(valid(b))
        def _():
            for cp in copies(b):
                cp.wait_recv()
            for cp in copies(b):
                cp.wait_send()

    def out_gate_up(b):
        a = ring(b, 2)
        l, m = layer_of(b), block_of(rem(b, nj))
        cps = []
        for gu, out in enumerate((dg_ref, du_ref)):
            for hf in range(2):
                cols = pl.ds(pl.multiple_of(hf * half + m * 128, 128), 128)
                src = fog.at[a, gu, :, pl.ds(hf * 128, 128)]
                cps.append(pltpu.make_async_copy(src, out.at[l, :, cols], o_sem.at[gu * 2 + hf, a]))
        return cps

    def out_down(b, own):
        a, r = ring(b, 2), ring(b, 8)
        core, piece = owner_piece(rem(b, nj), c)
        dst = dd_ref.at[layer_of(b), pl.ds(pl.multiple_of(piece * 64, 64), 64)]
        if own:
            return pltpu.make_async_copy(fod.at[a], dst, f_loc.at[a])
        return remote(fod.at[a], dst, f_snd.at[r], f_rcv.at[r], partner)

    def out_start(b, cond=None):
        ok = valid(b) if cond is None else valid(b) & cond
        core, _ = owner_piece(rem(b + BASE * nj, nj), c)

        @pl.when(ok)
        def _():
            for cp in out_gate_up(b):
                cp.start()

        @pl.when(ok & (core == c))
        def _():
            out_down(b, True).start()

        @pl.when(ok & (core != c))
        def _():
            out_down(b, False).start()

    def out_wait(b):
        @pl.when(valid(b))
        def _():
            for cp in out_gate_up(b):
                cp.wait()
            core, _ = owner_piece(rem(b, nj), c)
            theirs, _ = owner_piece(rem(b, nj), 1 - c)

            @pl.when(core == c)
            def _():
                out_down(b, True).wait()

            @pl.when(core != c)
            def _():
                out_down(b, False).wait_send()

            @pl.when(theirs == c)
            def _():
                out_down(b, False).wait_recv()

    def sum_y(b):
        a, z = ring(b, 2), ring(b, 4)
        for i in range(2):
            fog[a, i] = ysg[a, i] + ryg[z, i]
        fod[a] = ysd[a] + ryd[z]

    def sum_x(b):
        a, z = ring(b, 2), ring(b, 4)
        for i in range(2):
            ysg[a, i] = pog[a, i] + rxg[z, i]
        ysd[a] = pod[a] + rxd[z]

    def sum_cores(b):
        a = ring(b, 2)
        for i in range(2):
            pog[a, i] = sg[a, i, x, c] + rdg[a, i, x]
            xsg[a, i] = sg[a, i, 1 - x, c] + rdg[a, i, 1 - x]
        pod[a] = sd[a, x, c] + rdd[a, x]
        xsd[a] = sd[a, 1 - x, c] + rdd[a, 1 - x]

    def ahead(s):
        return (s > steps - SHORT).astype(jnp.int32)

    def front(s, sent):
        sent = (next_piece(s + LEAD, sent[0]), *sent[:-1])

        @pl.when((s + 1 >= 0) & (s + 1 < steps))
        def _():
            load_weights(s + 1, False)

        k = ahead(s)
        wait_all(core_copies, s - 2)
        wait_all(x_copies, s - 4 + k)
        wait_all(y_copies, s - 6 + k)
        out_wait(s - 8 + k)

        full = (s >= 6) & (s < steps - SHORT)

        @pl.when(full)
        def _():
            sum_y(s - 6)
            sum_x(s - 4)
            sum_cores(s - 2)

        for f, b in ((sum_y, s - 6 + k), (sum_x, s - 4 + k)):
            @pl.when(valid(b) & ((s < 6) | (s >= steps - SHORT)))
            def _():
                f(b)

        @pl.when(s == steps - SHORT)
        def _():
            wait_all(x_copies, s - 3)
            wait_all(y_copies, s - 5)
            out_wait(s - 7)
            sum_y(s - 5)
            sum_x(s - 3)

        @pl.when(valid(s - 2) & ((s < 6) | (s >= steps - SHORT)))
        def _():
            sum_cores(s - 2)

        weights_wait(sent)
        return sent

    def starts(s, sent, cond=None):
        k = ahead(s)

        def also(c):
            return c if cond is None else c & cond

        if cond is None:
            weights_send(sent)
        else:
            for i, kinds in ((0, "BA"), (2, "CD"), (4, "E")):
                @pl.when(also(sent[i] > sent[i + 1]))
                def _():
                    weight_start(kinds, sent[i + 1])

        start_all(core_copies, s - 1, cond)
        start_all(x_copies, s - 2, cond)
        start_all(y_copies, s - 4 + k, cond)
        out_start(s - 6 + k, cond)

        @pl.when(also((s + 2 >= 0) & (s + 2 < steps)))
        def _():
            load_weights(s + 2, True)

        @pl.when(also(s == steps - SHORT))
        def _():
            start_all(y_copies, s - 3)
            out_start(s - 5)

    def boundary(s, sent):
        sent = front(s, sent)
        starts(s, sent)
        return sent

    blocks = tokens // tb

    def prepare(s):
        for i in range(2):
            hb[0, i] = wgu_b[ring(s, 3), i].T

    def first(s, t):
        tok = pl.ds(t * tb, tb)
        u = dot(hb[0, 0], n_t[:, tok])
        v = dot(hb[0, 1], n_t[:, tok])
        da = dot(wd_b[ring(s, 3)], gb_t[:, tok])
        sig = jax.nn.sigmoid(u)
        silu = u * sig
        s_a[t % 2] = (silu * v).astype(BF16)
        s_du[t % 2] = (da * v * sig * (1.0 + u * (1.0 - sig))).astype(BF16)
        s_dv[t % 2] = (da * silu).astype(BF16)

    def second(s, t):
        tok = pl.ds(t * tb, tb)
        slot, w = ring(s, 2), ring(s, 3)
        for i, val in enumerate((s_du, s_dv)):
            part = dot_nt(n_t[:, tok], val[t % 2])
            if t > 0:
                part = acc[i] + part
            if t < blocks - 1:
                acc[i] = part
            else:
                sg[slot, i] = part.reshape(2, 2, dq, FB)
        part = dot_nt(gb_t[:, tok], s_a[t % 2])
        if t > 0:
            part = acc[2] + part
        if t < blocks - 1:
            acc[2] = part
        else:
            sd[slot] = part.T.reshape(2, 2, 64, width)
        dn_t[:, tok] += dot(wgu_b[w, 0], s_du[t % 2]) + dot(wgu_b[w, 1], s_dv[t % 2])

    def compute(s):
        for t in range(1, blocks):
            first(s, t)
            second(s, t - 1)
        prepare(s + 1)
        first(s + 1, 0)
        second(s, blocks - 1)

    n_tok = tokens // nb

    def tok_of(i):
        return pl.ds(pl.multiple_of(i * nb, nb), nb)

    def rows_load(i, src, which):
        return pltpu.make_async_copy(src.at[tok_of(i)], hb.at[ring(i, 2), which], hb_sem.at[ring(i, 2), which])

    def g_load(i):
        return pltpu.make_async_copy(gt_ref.at[:, tok_of(i)], acc.at[ring(i, 3)], gl_sem.at[ring(i, 3)])

    def g_store(i):
        return pltpu.make_async_copy(acc.at[ring(i, 3)], gt_ref.at[:, tok_of(i)], gs_sem.at[ring(i, 3)])

    groups = [pl.ds(k, 128) for k in range(0, width, 128)]

    def new_norm(i):
        tok = tok_of(i)
        total = jnp.zeros((1, nb), F32)
        for rows in groups:
            xt = hb[ring(i, 2), 1, :, rows].T
            n_t[rows, tok] = xt
            xf = xt.astype(F32)
            total += jnp.sum(xf * xf, axis=0, keepdims=True)
        r = lax.rsqrt(total * (1.0 / width) + EPS)
        r_row[:, tok] = r
        for rows in groups:
            n_t[rows, tok] = (n_t[rows, tok].astype(F32) * r).astype(BF16)
            dn_t[rows, tok] = jnp.zeros((128, nb), F32)

    def new_g(i, put):
        tok = tok_of(i)
        r = r_row[:, tok]
        total = jnp.zeros((1, nb), F32)
        for rows in groups:
            xt = hb[ring(i, 2), 0, :, rows].T
            gb_t[rows, tok] = xt
            total += jnp.sum(dn_t[rows, tok] * (xt.astype(F32) * r), axis=0, keepdims=True)
        m = total * (1.0 / width)
        for rows in groups:
            nf = gb_t[rows, tok].astype(F32) * r
            put(rows, acc[ring(i, 3), rows] + r * (dn_t[rows, tok] - nf * m))

    def enter_block(i):
        h_new = h_ref.at[layers - 1]

        @pl.when(i == 0)
        def _():
            rows_load(i, g_ref, 0).start()
            rows_load(i, h_new, 1).start()

        @pl.when(i + 1 < n_tok)
        def _():
            rows_load(i + 1, g_ref, 0).start()
            rows_load(i + 1, h_new, 1).start()

        @pl.when(i >= 3)
        def _():
            g_store(i - 3).wait()

        rows_load(i, g_ref, 0).wait()
        rows_load(i, h_new, 1).wait()
        for rows in groups:
            gb = hb[ring(i, 2), 0, :, rows].T
            gb_t[rows, tok_of(i)] = gb
            acc[ring(i, 3), rows] = gb.astype(F32)
        new_norm(i)
        g_store(i).start()

    def stores_done():
        for i in range(n_tok - 3, n_tok):
            g_store(i).wait()

    def between(l_new):
        h_old, h_new = h_ref.at[l_new + 1], h_ref.at[l_new]
        rows_load(0, h_old, 0).start()
        rows_load(0, h_new, 1).start()
        g_load(0).start()

        def body(i, _):
            @pl.when(i >= 2)
            def _():
                g_store(i - 2).wait()

            @pl.when(i + 1 < n_tok)
            def _():
                rows_load(i + 1, h_old, 0).start()
                rows_load(i + 1, h_new, 1).start()
                g_load(i + 1).start()

            rows_load(i, h_old, 0).wait()
            rows_load(i, h_new, 1).wait()
            g_load(i).wait()

            def put(rows, g):
                acc[ring(i, 3), rows] = g
                gb_t[rows, tok_of(i)] = g.astype(BF16)

            new_g(i, put)
            new_norm(i)
            g_store(i).start()
            return 0

        lax.fori_loop(0, n_tok, body, 0)
        for i in range(n_tok - 2, n_tok):
            g_store(i).wait()

    def leave():
        h_old = h_ref.at[0]

        def dh_store(i):
            return pltpu.make_async_copy(hb.at[ring(i, 2), 1], dh_ref.at[tok_of(i)], do_sem.at[ring(i, 2)])

        rows_load(0, h_old, 0).start()
        g_load(0).start()

        def body(i, _):
            @pl.when(i + 1 < n_tok)
            def _():
                rows_load(i + 1, h_old, 0).start()
                g_load(i + 1).start()

            @pl.when(i >= 2)
            def _():
                dh_store(i - 2).wait()

            rows_load(i, h_old, 0).wait()
            g_load(i).wait()

            def put(rows, g):
                hb[ring(i, 2), 1, :, rows] = g.astype(BF16).T

            new_g(i, put)
            dh_store(i).start()
            return 0

        lax.fori_loop(0, n_tok, body, 0)
        for i in range(n_tok - 2, n_tok):
            dh_store(i).wait()

    barrier = pltpu.get_barrier_semaphore()
    for dev in (partner, x_dev, y_dev):
        pl.semaphore_signal(barrier, inc=1, device_id=dev, device_id_type=MESH)
    pl.semaphore_wait(barrier, 3)

    per = n_tok // (LEAD - 1)

    def lead_in(i, sent):
        sent = boundary(i - LEAD, sent)

        @pl.when(i < LEAD - 1)
        def _():
            for k in range(per):
                enter_block(i * per + k)

        return sent

    sent = lax.fori_loop(0, LEAD, lead_in, (jnp.int32(0),) * 8)
    stores_done()

    def main(s, sent):
        sent = front(s, sent)
        apart = (rem(s, nj) == 0) | (s < LEAD)

        @pl.when(apart)
        def _():
            starts(s, sent)

        @pl.when(rem(s, nj) == 0)
        def _():
            @pl.when(s > 0)
            def _():
                between(layer_of(s))

            prepare(s)
            first(s, 0)

        starts(s, sent, jnp.logical_not(apart))
        compute(s)
        return sent

    sent = lax.fori_loop(0, steps, main, sent)
    sent = lax.fori_loop(steps, steps + 2, boundary, sent)
    leave()
    lax.fori_loop(steps + 2, steps + 7, boundary, sent)


def backward(dims, h, g, gate, up, wd):
    layers, tokens, width, hidden, tb, nb = dims
    dq = width // 4
    nj = hidden // FB
    steps = layers * nj
    dma = pltpu.SemaphoreType.DMA
    vm = pltpu.VMEM
    anyspace = pl.BlockSpec(memory_space=pl.ANY)
    sds = jax.ShapeDtypeStruct
    out_shape = [
        sds((layers, dq, hidden), F32),
        sds((layers, dq, hidden), F32),
        sds((layers, hidden // 4, width), F32),
        sds((tokens, width), BF16),
        sds((steps, 4, 2, dq, FB), BF16),
        sds((steps, 4, 64, width), BF16),
        sds((width, tokens), F32),
    ]

    def pair(n):
        return [vm((n, 2, dq, FB), F32), vm((n, 64, width), F32)]

    scratch = [
        vm((width, tokens), BF16),
        vm((width, tokens), BF16),
        vm((width, tokens), F32),
        vm((1, tokens), F32),
        vm((3, 2, width, FB), BF16),
        vm((3, FB, width), BF16),
        vm((2, FB, tb), BF16),
        vm((2, FB, tb), BF16),
        vm((2, FB, tb), BF16),
        vm((3, width, FB), F32),
        vm((2, 2, nb, width), BF16),
        vm((2, 2, 2, 2, dq, FB), F32),
        vm((2, 2, 2, 64, width), F32),
        vm((2, 2, 2, dq, FB), F32),
        vm((2, 2, 64, width), F32),
        *pair(2), *pair(2), *pair(4), *pair(2), *pair(4), *pair(2),
        dma((3, 8)),
        dma((2, 8)), dma((2, 8)), dma((2, 8)), dma((2, 8)), dma((2, 8)), dma((2, 8)),
        dma((4, 2)), dma((2,)), dma((8,)), dma((8,)),
        dma((5, 2, RS)), dma((5, 2, RS)),
        dma((2, 2)), dma((3,)), dma((3,)), dma((2,)),
    ]
    return pl.pallas_call(
        functools.partial(kernel, dims),
        out_shape=out_shape,
        in_specs=[anyspace] * 5,
        out_specs=[anyspace] * 7,
        scratch_shapes=scratch,
        compiler_params=pltpu.CompilerParams(
            collective_id=0, has_side_effects=True, vmem_limit_bytes=67043328,
        ),
        name="mlp_backward",
    )(h, g, gate, up, wd)[:4]


def solution(mesh):
    tok_spec = P(("dp", "fsdp"))
    stack_spec = P(None, ("dp", "fsdp"))
    weight_spec = P(None, "fsdp")

    def local_backward(h_saved, grad_out, gate_sh, up_sh, down_sh):
        layers = h_saved.shape[0]
        b_loc, seq, width = grad_out.shape
        tokens = b_loc * seq
        dq, hidden = gate_sh.shape[1:]
        nj = hidden // FB
        tb = min(512, tokens // 2)
        nb = FB
        wd = down_sh.reshape(layers, nj, 64, width)
        dims = (layers, tokens, width, hidden, tb, nb)
        d_gate, d_up, d_down, d_h0 = backward(
            dims, h_saved.reshape(layers, tokens, width), grad_out.reshape(tokens, width), gate_sh, up_sh, wd
        )
        return d_gate, d_up, d_down, d_h0.reshape(b_loc, seq, width)

    return jax.shard_map(
        local_backward,
        mesh=mesh,
        in_specs=(stack_spec, tok_spec, weight_spec, weight_spec, weight_spec),
        out_specs=(weight_spec, weight_spec, weight_spec, tok_spec),
        check_vma=False,
    )
```

```python
import functools

import jax
import jax.numpy as jnp
from jax import lax
from jax.experimental import pallas as pl
from jax.experimental.pallas import tpu as pltpu
from jax.sharding import PartitionSpec as P

EPS = 1e-5
MESH = pl.DeviceIdType.MESH
F32 = jnp.float32
BF16 = jnp.bfloat16
FB = 256
LEAD = 9
BURST = 6
RS = 32
AHEAD = 3
SHORT = 6
BASE = 240
DOT_NT = (((1,), (1,)), ((), ()))


def div(a, b):
    return a // b if isinstance(a, int) else lax.div(a, jnp.int32(b))


def rem(a, b):
    return a % b if isinstance(a, int) else lax.rem(a, jnp.int32(b))


def ring(i, n):
    return rem(i + BASE, n)


def dot(a, b):
    return jnp.dot(a, b, preferred_element_type=F32)


def dot_nt(a, b):
    return lax.dot_general(a, b, DOT_NT, preferred_element_type=F32)


def kernel(
    dims, h_ref, g_ref, gate_ref, up_ref, wd_ref,
    dg_ref, du_ref, dd_ref, dh_ref, ggu, gwd, gt_ref,
    n_t, gb_t, dn_t, r_row, wgu_b, wd_b, s_a, s_du, s_dv, acc, hb,
    sg, sd, rdg, rdd, xsg, xsd, pog, pod, rxg, rxd, ysg, ysd, ryg, ryd, fog, fod,
    wl_sem, d_snd, d_rcv, x_snd, x_rcv, y_snd, y_rcv, o_sem, f_loc, f_snd, f_rcv,
    w_snd, w_rcv, hb_sem, gl_sem, gs_sem, do_sem,
):
    layers, tokens, width, hidden, tb, nb = dims
    dq = width // 4
    hq = dq // 2
    half = hidden // 2
    nj = hidden // FB
    mid = nj // 2
    steps = layers * nj
    y = lax.axis_index("dp")
    me = lax.axis_index("fsdp")
    x = me // 2
    c = me % 2
    qx = (1 - x) * 2 + c
    partner = (y, x * 2 + 1 - c)
    x_dev = (y, qx)
    y_dev = (1 - y, me)

    def layer_of(s):
        return layers - 1 - div(s, nj)

    def block_of(t):
        return div(t, 2) + rem(t, 2) * (mid + 1)

    def owner_piece(t, e):
        last = div(t, nj - 1)
        core = (1 - last) * rem(t, 2) + last * e
        piece = (1 - last) * (t + e) + last * (nj - 1) * (1 - e)
        return core, piece

    def remote(src, dst, snd, rcv, dev):
        return pltpu.make_async_remote_copy(
            src_ref=src, dst_ref=dst, send_sem=snd, recv_sem=rcv, device_id=dev, device_id_type=MESH
        )

    def next_piece(beta, n):
        burst = ((beta >= LEAD) & (beta < LEAD + 3)).astype(jnp.int32)
        skip = ((beta >= LEAD + 3) & (rem(beta, 5) == 4)).astype(jnp.int32)
        return n + (1 + (BURST - 1) * burst - skip) * (n < steps).astype(jnp.int32)

    def shard_parts(l, t, rows):
        m = block_of(t)
        for gu, ref in enumerate((gate_ref, up_ref)):
            for hf in range(2):
                cols = pl.ds(pl.multiple_of(hf * half + m * 128, 128), 128)
                yield ref.at[l, rows, cols], gu, pl.ds(hf * 128, 128)

    def weight_copies(kind, p, whole):
        l, t = layer_of(p), rem(p, nj)
        rs = ring(p, RS)
        k = "ABCDE".index(kind)
        q = me if kind in "AB" else qx
        dev = {"A": partner, "B": x_dev, "C": y_dev, "D": partner, "E": partner}[kind]
        if kind == "A":
            rows, rows_d = pl.ds(0, dq), pl.ds(0, 64)
        else:
            side = 1 - y if kind == "E" else y
            rows = pl.ds(pl.multiple_of(side * hq, 16), hq)
            rows_d = pl.ds(pl.multiple_of(side * 32, 32), 32)
        sems = w_snd.at[k, 0, rs], w_rcv.at[k, 0, rs]
        if kind in "AB" and not whole:
            for src, gu, lanes in shard_parts(l, t, rows):
                yield remote(src, ggu.at[p, q, gu, rows, lanes], *sems, dev)
        else:
            both = ggu.at[p, q, :, rows]
            yield remote(both, both, *sems, dev)
        wd_dst = gwd.at[p, q, rows_d]
        wd_src = wd_ref.at[l, t, rows_d] if kind in "AB" else wd_dst
        yield remote(wd_src, wd_dst, w_snd.at[k, 1, rs], w_rcv.at[k, 1, rs], dev)

    def pieces(span, act):
        def body(p, _):
            act(p)
            return 0

        lax.fori_loop(*span, body, 0)

    def weight_start(kinds, p):
        for kind in kinds:
            for cp in weight_copies(kind, p, False):
                cp.start()

    def weight_wait_recv(kinds, p):
        for kind in kinds:
            for cp in weight_copies(kind, p, True):
                cp.wait_recv()

    def weight_wait_send(kinds, p):
        for kind in kinds:
            for cp in weight_copies(kind, p, True):
                cp.wait_send()

    def weights_wait(sent):
        def arrived_x(p):
            weight_wait_recv("B", p)
            weight_wait_send("AB", p)

        def arrived_y(p):
            weight_wait_recv("C", p)
            weight_wait_send("CD", p)

        def complete(p):
            weight_wait_recv("ADE", p)
            weight_wait_send("E", p)

        pieces((sent[3], sent[2]), arrived_x)
        pieces((sent[5], sent[4]), arrived_y)
        pieces((sent[7], sent[6]), complete)

    def weights_send(sent):
        pieces((sent[1], sent[0]), functools.partial(weight_start, "BA"))
        pieces((sent[3], sent[2]), functools.partial(weight_start, "CD"))
        pieces((sent[5], sent[4]), functools.partial(weight_start, "E"))

    def weight_loads(s):
        slot = ring(s, 3)
        l, t = layer_of(s), rem(s, nj)

        def copy(src, dst, i):
            return pltpu.make_async_copy(src, dst, wl_sem.at[slot, i])

        for d in range(4):
            q = rem(me + d, 4)
            rows = pl.ds(pl.multiple_of(q * dq, 16), dq)
            if d == 0:
                for src, gu, lanes in shard_parts(l, t, pl.ds(0, dq)):
                    yield True, copy(src, wgu_b.at[slot, gu, rows, lanes], 0)
            else:
                yield True, copy(ggu.at[s, q], wgu_b.at[slot, :, rows], 0)
        for e in range(2):
            core, piece = owner_piece(t, e)
            for xx in range(2):
                q = xx * 2 + core
                dst = wd_b.at[slot, pl.ds(xx * 128 + e * 64, 64)]
                yield q == me, copy(wd_ref.at[l, piece], dst, 1)
                yield q != me, copy(gwd.at[s - t + piece, q], dst, 1)

    def load_start(s, cond):
        for mine, cp in weight_loads(s):
            start_if(cond & mine, [cp])

    def load_wait(s):
        slot = ring(s, 3)
        for i, buf in enumerate((wgu_b, wd_b)):
            pltpu.make_async_copy(buf.at[slot], buf.at[slot], wl_sem.at[slot, i]).wait()

    def core_copies(b):
        r, a, z = ring(b, 8), ring(b, 2), ring(b, 2)
        return (
            remote(sg.at[a, :, :, 1 - c], rdg.at[z], d_snd.at[0, r], d_rcv.at[0, r], partner),
            remote(sd.at[a, :, 1 - c], rdd.at[z], d_snd.at[1, r], d_rcv.at[1, r], partner),
        )

    def x_copies(b):
        r, a, z = ring(b, 8), ring(b, 2), ring(b, 4)
        return (
            remote(xsg.at[a], rxg.at[z], x_snd.at[0, r], x_rcv.at[0, r], x_dev),
            remote(xsd.at[a], rxd.at[z], x_snd.at[1, r], x_rcv.at[1, r], x_dev),
        )

    def y_copies(b):
        r, a, z = ring(b, 8), ring(b, 2), ring(b, 4)
        return (
            remote(ysg.at[a], ryg.at[z], y_snd.at[0, r], y_rcv.at[0, r], y_dev),
            remote(ysd.at[a], ryd.at[z], y_snd.at[1, r], y_rcv.at[1, r], y_dev),
        )

    def valid(b):
        return (b >= 0) & (b < steps)

    def start_if(cond, copies):
        for cp in copies:
            @pl.when(cond)
            def _():
                cp.start()

    def start_all(copies, b, cond=None):
        start_if(valid(b) if cond is None else valid(b) & cond, copies(b))

    def wait_all(copies, b):
        @pl.when(valid(b))
        def _():
            for cp in copies(b):
                cp.wait_recv()
            for cp in copies(b):
                cp.wait_send()

    def out_gate_up(b):
        a = ring(b, 2)
        l, m = layer_of(b), block_of(rem(b, nj))
        cps = []
        for gu, out in enumerate((dg_ref, du_ref)):
            for hf in range(2):
                cols = pl.ds(pl.multiple_of(hf * half + m * 128, 128), 128)
                src = fog.at[a, gu, :, pl.ds(hf * 128, 128)]
                cps.append(pltpu.make_async_copy(src, out.at[l, :, cols], o_sem.at[gu * 2 + hf, a]))
        return cps

    def out_down(b, own):
        a, r = ring(b, 2), ring(b, 8)
        core, piece = owner_piece(rem(b, nj), c)
        dst = dd_ref.at[layer_of(b), pl.ds(pl.multiple_of(piece * 64, 64), 64)]
        if own:
            return pltpu.make_async_copy(fod.at[a], dst, f_loc.at[a])
        return remote(fod.at[a], dst, f_snd.at[r], f_rcv.at[r], partner)

    def out_start(b, cond=None):
        ok = valid(b) if cond is None else valid(b) & cond
        core, _ = owner_piece(rem(b + BASE * nj, nj), c)

        start_if(ok, out_gate_up(b))
        start_if(ok & (core == c), [out_down(b, True)])
        start_if(ok & (core != c), [out_down(b, False)])

    def out_wait(b):
        @pl.when(valid(b))
        def _():
            for cp in out_gate_up(b):
                cp.wait()
            core, _ = owner_piece(rem(b, nj), c)
            theirs, _ = owner_piece(rem(b, nj), 1 - c)

            @pl.when(core == c)
            def _():
                out_down(b, True).wait()

            @pl.when(core != c)
            def _():
                out_down(b, False).wait_send()

            @pl.when(theirs == c)
            def _():
                out_down(b, False).wait_recv()

    def sum_y(b):
        a, z = ring(b, 2), ring(b, 4)
        for i in range(2):
            fog[a, i] = ysg[a, i] + ryg[z, i]
        fod[a] = ysd[a] + ryd[z]

    def sum_x(b):
        a, z = ring(b, 2), ring(b, 4)
        for i in range(2):
            ysg[a, i] = pog[a, i] + rxg[z, i]
        ysd[a] = pod[a] + rxd[z]

    def sum_cores(b):
        a = ring(b, 2)
        for i in range(2):
            pog[a, i] = sg[a, i, x, c] + rdg[a, i, x]
            xsg[a, i] = sg[a, i, 1 - x, c] + rdg[a, i, 1 - x]
        pod[a] = sd[a, x, c] + rdd[a, x]
        xsd[a] = sd[a, 1 - x, c] + rdd[a, 1 - x]

    def ahead(s):
        return (s > steps - SHORT).astype(jnp.int32)

    def front(s, sent):
        sent = (next_piece(s + LEAD, sent[0]), *sent[:-1])

        @pl.when((s + 1 >= 0) & (s + 1 < steps))
        def _():
            load_wait(s + 1)

        k = ahead(s)
        wait_all(core_copies, s - 2)
        wait_all(x_copies, s - 4 + k)
        wait_all(y_copies, s - 6 + k)
        out_wait(s - 8 + k)

        full = (s >= 6) & (s < steps - SHORT)

        @pl.when(full)
        def _():
            sum_y(s - 6)
            sum_x(s - 4)
            sum_cores(s - 2)

        for f, b in ((sum_y, s - 6 + k), (sum_x, s - 4 + k)):
            @pl.when(valid(b) & ((s < 6) | (s >= steps - SHORT)))
            def _():
                f(b)

        @pl.when(s == steps - SHORT)
        def _():
            wait_all(x_copies, s - 3)
            wait_all(y_copies, s - 5)
            out_wait(s - 7)
            sum_y(s - 5)
            sum_x(s - 3)

        @pl.when(valid(s - 2) & ((s < 6) | (s >= steps - SHORT)))
        def _():
            sum_cores(s - 2)

        @pl.when(s < LEAD)
        def _():
            weights_wait(sent)

        for i, recv, send in ((2, "B", "AB"), (4, "C", "CD"), (6, "ADE", "E")):
            @pl.when((s >= LEAD) & (sent[i] > sent[i + 1]))
            def _():
                weight_wait_recv(recv, sent[i + 1])
                weight_wait_send(send, sent[i + 1])

        return sent

    def starts(s, sent, cond=None):
        k = ahead(s)

        def also(c):
            return c if cond is None else c & cond

        if cond is None:
            weights_send(sent)
        else:
            for i, kinds in ((0, "BA"), (2, "CD"), (4, "E")):
                for kind in kinds:
                    start_if(also(sent[i] > sent[i + 1]), weight_copies(kind, sent[i + 1], False))

        start_all(core_copies, s - 1, cond)
        start_all(x_copies, s - 2, cond)
        start_all(y_copies, s - 4 + k, cond)
        out_start(s - 6 + k, cond)

        load_start(s + 2, also(valid(s + 2)))
        last = s == steps - SHORT
        start_all(y_copies, s - 3, also(last))
        out_start(s - 5, also(last))

    def boundary(s, sent):
        sent = front(s, sent)
        starts(s, sent)
        return sent

    blocks = tokens // tb

    def prepare(s):
        for i in range(2):
            hb[0, i] = wgu_b[ring(s, 3), i].T

    def first(s, t):
        tok = pl.ds(t * tb, tb)
        u = dot(hb[0, 0], n_t[:, tok])
        v = dot(hb[0, 1], n_t[:, tok])
        da = dot(wd_b[ring(s, 3)], gb_t[:, tok])
        sig = jax.nn.sigmoid(u)
        silu = u * sig
        s_a[t % 2] = (silu * v).astype(BF16)
        s_du[t % 2] = (da * v * sig * (1.0 + u * (1.0 - sig))).astype(BF16)
        s_dv[t % 2] = (da * silu).astype(BF16)

    def second(s, t):
        tok = pl.ds(t * tb, tb)
        slot, w = ring(s, 2), ring(s, 3)
        for i, val in enumerate((s_du, s_dv)):
            part = dot_nt(n_t[:, tok], val[t % 2])
            if t > 0:
                part = acc[i] + part
            if t < blocks - 1:
                acc[i] = part
            else:
                sg[slot, i] = part.reshape(2, 2, dq, FB)
        part = dot_nt(gb_t[:, tok], s_a[t % 2])
        if t > 0:
            part = acc[2] + part
        if t < blocks - 1:
            acc[2] = part
        else:
            sd[slot] = part.T.reshape(2, 2, 64, width)
        dn_t[:, tok] += dot(wgu_b[w, 0], s_du[t % 2]) + dot(wgu_b[w, 1], s_dv[t % 2])

    def compute(s):
        for t in range(1, blocks):
            first(s, t)
            second(s, t - 1)
        prepare(s + 1)
        first(s + 1, 0)
        second(s, blocks - 1)

    n_tok = tokens // nb
    groups = [pl.ds(k, 128) for k in range(0, width, 128)]

    def tok_of(i):
        return pl.ds(pl.multiple_of(i * nb, nb), nb)

    def rows_buf(i, which):
        k = ring(i, 4)
        return hb.at[div(k, 2), which, pl.ds(pl.multiple_of(rem(k, 2) * nb, nb), nb)]

    def g_buf(i):
        k = ring(i, 6)
        return acc.at[div(k, 2), :, pl.ds(pl.multiple_of(rem(k, 2) * nb, nb), nb)]

    def rows_load(i, src, which):
        return pltpu.make_async_copy(src.at[tok_of(i)], rows_buf(i, which), hb_sem.at[ring(i, 4), which])

    def g_load(i):
        return pltpu.make_async_copy(gt_ref.at[:, tok_of(i)], g_buf(i), gl_sem.at[ring(i, 6)])

    def g_store(i):
        return pltpu.make_async_copy(g_buf(i), gt_ref.at[:, tok_of(i)], gs_sem.at[ring(i, 6)])

    def new_norm(i):
        tok, buf = tok_of(i), rows_buf(i, 1)
        total = jnp.zeros((1, nb), F32)
        for rows in groups:
            xt = buf[:, rows].T
            n_t[rows, tok] = xt
            xf = xt.astype(F32)
            total += jnp.sum(xf * xf, axis=0, keepdims=True)
        r = lax.rsqrt(total * (1.0 / width) + EPS)
        r_row[:, tok] = r
        for rows in groups:
            n_t[rows, tok] = (n_t[rows, tok].astype(F32) * r).astype(BF16)
            dn_t[rows, tok] = jnp.zeros((128, nb), F32)

    def new_g(i, put):
        tok, buf, g = tok_of(i), rows_buf(i, 0), g_buf(i)
        r = r_row[:, tok]
        total = jnp.zeros((1, nb), F32)
        for rows in groups:
            xt = buf[:, rows].T
            gb_t[rows, tok] = xt
            total += jnp.sum(dn_t[rows, tok] * (xt.astype(F32) * r), axis=0, keepdims=True)
        m = total * (1.0 / width)
        for rows in groups:
            nf = gb_t[rows, tok].astype(F32) * r
            put(rows, g[rows] + r * (dn_t[rows, tok] - nf * m))

    def fetch(loads, i):
        @pl.when(i == 0)
        def _():
            for k in range(AHEAD):
                for ld in loads:
                    ld(k).start()

        @pl.when(i + AHEAD < n_tok)
        def _():
            for ld in loads:
                ld(i + AHEAD).start()

        for ld in loads:
            ld(i).wait()

    def enter_block(i):
        @pl.when(i >= 6)
        def _():
            g_store(i - 6).wait()

        fetch([lambda k: rows_load(k, g_ref, 0), lambda k: rows_load(k, h_ref.at[layers - 1], 1)], i)
        buf, g = rows_buf(i, 0), g_buf(i)
        for rows in groups:
            gb = buf[:, rows].T
            gb_t[rows, tok_of(i)] = gb
            g[rows] = gb.astype(F32)
        new_norm(i)
        g_store(i).start()

    def stores_done(last):
        for i in range(n_tok - last, n_tok):
            g_store(i).wait()

    def between(l_new):
        loads = [lambda k: rows_load(k, h_ref.at[l_new + 1], 0), lambda k: rows_load(k, h_ref.at[l_new], 1), g_load]

        def body(i, _):
            @pl.when(i >= 6 - AHEAD)
            def _():
                g_store(i - (6 - AHEAD)).wait()

            fetch(loads, i)

            def put(rows, g):
                g_buf(i)[rows] = g
                gb_t[rows, tok_of(i)] = g.astype(BF16)

            new_g(i, put)
            new_norm(i)
            g_store(i).start()
            return 0

        lax.fori_loop(0, n_tok, body, 0)
        stores_done(6 - AHEAD)

    def leave():
        def dh_store(i):
            return pltpu.make_async_copy(rows_buf(i, 1), dh_ref.at[tok_of(i)], do_sem.at[ring(i, 4)])

        def body(i, _):
            fetch([lambda k: rows_load(k, h_ref.at[0], 0), g_load], i)

            @pl.when(i >= 4)
            def _():
                dh_store(i - 4).wait()

            def put(rows, g):
                rows_buf(i, 1)[:, rows] = g.astype(BF16).T

            new_g(i, put)
            dh_store(i).start()
            return 0

        lax.fori_loop(0, n_tok, body, 0)
        for i in range(n_tok - 4, n_tok):
            dh_store(i).wait()

    barrier = pltpu.get_barrier_semaphore()
    for dev in (partner, x_dev, y_dev):
        pl.semaphore_signal(barrier, inc=1, device_id=dev, device_id_type=MESH)
    pl.semaphore_wait(barrier, 3)

    per = n_tok // (LEAD - 1)

    def lead_in(i, sent):
        sent = boundary(i - LEAD, sent)

        @pl.when(i < LEAD - 1)
        def _():
            for k in range(per):
                enter_block(i * per + k)

        return sent

    sent = lax.fori_loop(0, LEAD, lead_in, (jnp.int32(0),) * 8)
    stores_done(6)

    def main(s, sent):
        sent = front(s, sent)
        apart = (rem(s, nj) == 0) | (s < LEAD)

        @pl.when(apart)
        def _():
            starts(s, sent)

        @pl.when(rem(s, nj) == 0)
        def _():
            @pl.when(s > 0)
            def _():
                between(layer_of(s))

            prepare(s)
            first(s, 0)

        starts(s, sent, jnp.logical_not(apart))
        compute(s)
        return sent

    sent = lax.fori_loop(0, steps, main, sent)
    sent = lax.fori_loop(steps, steps + 2, boundary, sent)
    leave()
    lax.fori_loop(steps + 2, steps + 7, boundary, sent)


def backward(dims, h, g, gate, up, wd):
    layers, tokens, width, hidden, tb, nb = dims
    dq = width // 4
    nj = hidden // FB
    steps = layers * nj
    dma = pltpu.SemaphoreType.DMA
    vm = pltpu.VMEM
    anyspace = pl.BlockSpec(memory_space=pl.ANY)
    sds = jax.ShapeDtypeStruct
    out_shape = [
        sds((layers, dq, hidden), F32),
        sds((layers, dq, hidden), F32),
        sds((layers, hidden // 4, width), F32),
        sds((tokens, width), BF16),
        sds((steps, 4, 2, dq, FB), BF16),
        sds((steps, 4, 64, width), BF16),
        sds((width, tokens), F32),
    ]

    def pair(n):
        return [vm((n, 2, dq, FB), F32), vm((n, 64, width), F32)]

    scratch = [
        vm((width, tokens), BF16),
        vm((width, tokens), BF16),
        vm((width, tokens), F32),
        vm((1, tokens), F32),
        vm((3, 2, width, FB), BF16),
        vm((3, FB, width), BF16),
        vm((2, FB, tb), BF16),
        vm((2, FB, tb), BF16),
        vm((2, FB, tb), BF16),
        vm((3, width, FB), F32),
        vm((2, 2, FB, width), BF16),
        vm((2, 2, 2, 2, dq, FB), F32),
        vm((2, 2, 2, 64, width), F32),
        vm((2, 2, 2, dq, FB), F32),
        vm((2, 2, 64, width), F32),
        *pair(2), *pair(2), *pair(4), *pair(2), *pair(4), *pair(2),
        dma((3, 2)),
        dma((2, 8)), dma((2, 8)), dma((2, 8)), dma((2, 8)), dma((2, 8)), dma((2, 8)),
        dma((4, 2)), dma((2,)), dma((8,)), dma((8,)),
        dma((5, 2, RS)), dma((5, 2, RS)),
        dma((4, 2)), dma((6,)), dma((6,)), dma((4,)),
    ]
    return pl.pallas_call(
        functools.partial(kernel, dims),
        out_shape=out_shape,
        in_specs=[anyspace] * 5,
        out_specs=[anyspace] * 7,
        scratch_shapes=scratch,
        compiler_params=pltpu.CompilerParams(
            collective_id=0, has_side_effects=True, vmem_limit_bytes=67043328,
        ),
        name="mlp_backward",
    )(h, g, gate, up, wd)[:4]


def solution(mesh):
    tok_spec = P(("dp", "fsdp"))
    stack_spec = P(None, ("dp", "fsdp"))
    weight_spec = P(None, "fsdp")

    def local_backward(h_saved, grad_out, gate_sh, up_sh, down_sh):
        layers = h_saved.shape[0]
        b_loc, seq, width = grad_out.shape
        tokens = b_loc * seq
        dq, hidden = gate_sh.shape[1:]
        nj = hidden // FB
        tb = min(512, tokens // 2)
        nb = 128
        wd = down_sh.reshape(layers, nj, 64, width)
        dims = (layers, tokens, width, hidden, tb, nb)
        d_gate, d_up, d_down, d_h0 = backward(
            dims, h_saved.reshape(layers, tokens, width), grad_out.reshape(tokens, width), gate_sh, up_sh, wd
        )
        return d_gate, d_up, d_down, d_h0.reshape(b_loc, seq, width)

    return jax.shard_map(
        local_backward,
        mesh=mesh,
        in_specs=(stack_spec, tok_spec, weight_spec, weight_spec, weight_spec),
        out_specs=(weight_spec, weight_spec, weight_spec, tok_spec),
        check_vma=False,
    )
```

```python
import functools

import jax
import jax.numpy as jnp
from jax import lax
from jax.experimental import pallas as pl
from jax.experimental.pallas import tpu as pltpu
from jax.sharding import PartitionSpec as P

EPS = 1e-5
MESH = pl.DeviceIdType.MESH
F32 = jnp.float32
BF16 = jnp.bfloat16
FB = 256
LEAD = 9
BURST = 4
RS = 32
SHORT = 6
BASE = 240
DOT_NT = (((1,), (1,)), ((), ()))


def div(a, b):
    return a // b if isinstance(a, int) else lax.div(a, jnp.int32(b))


def rem(a, b):
    return a % b if isinstance(a, int) else lax.rem(a, jnp.int32(b))


def ring(i, n):
    return rem(i + BASE, n)


def dot(a, b):
    return jnp.dot(a, b, preferred_element_type=F32)


def dot_nt(a, b):
    return lax.dot_general(a, b, DOT_NT, preferred_element_type=F32)


def kernel(
    dims, h_ref, g_ref, gate_ref, up_ref, wd_ref,
    dg_ref, du_ref, dd_ref, dh_ref, ggu, gwd, gt_ref,
    n_t, gb_t, dn_t, r_row, wgu_b, wd_b, s_a, s_du, s_dv, acc, hb,
    sg, sd, rdg, rdd, xsg, xsd, pog, pod, rxg, rxd, ysg, ysd, ryg, ryd, fog, fod,
    wl_sem, d_snd, d_rcv, x_snd, x_rcv, y_snd, y_rcv, o_sem, f_loc, f_snd, f_rcv,
    w_snd, w_rcv, hb_sem, gl_sem, gs_sem, do_sem,
):
    layers, tokens, width, hidden, tb, nb = dims
    dq = width // 4
    hq = dq // 2
    half = hidden // 2
    nj = hidden // FB
    mid = nj // 2
    steps = layers * nj
    y = lax.axis_index("dp")
    me = lax.axis_index("fsdp")
    x = me // 2
    c = me % 2
    qx = (1 - x) * 2 + c
    partner = (y, x * 2 + 1 - c)
    x_dev = (y, qx)
    y_dev = (1 - y, me)

    def layer_of(s):
        return layers - 1 - div(s, nj)

    def block_of(t):
        return div(t, 2) + rem(t, 2) * (mid + 1)

    def owner_piece(t, e):
        last = div(t, nj - 1)
        core = (1 - last) * rem(t, 2) + last * e
        piece = (1 - last) * (t + e) + last * (nj - 1) * (1 - e)
        return core, piece

    def remote(src, dst, snd, rcv, dev):
        return pltpu.make_async_remote_copy(
            src_ref=src, dst_ref=dst, send_sem=snd, recv_sem=rcv, device_id=dev, device_id_type=MESH
        )

    def next_piece(beta, n):
        burst = ((beta >= LEAD) & (beta < LEAD + 3)).astype(jnp.int32)
        skip = ((beta >= LEAD + 3) & (rem(beta, 7) == 4)).astype(jnp.int32)
        return n + (1 + (BURST - 1) * burst - skip) * (n < steps).astype(jnp.int32)

    def shard_parts(l, t, rows):
        m = block_of(t)
        for gu, ref in enumerate((gate_ref, up_ref)):
            for hf in range(2):
                cols = pl.ds(pl.multiple_of(hf * half + m * 128, 128), 128)
                yield ref.at[l, rows, cols], gu, pl.ds(hf * 128, 128)

    def weight_copies(kind, p, whole):
        l, t = layer_of(p), rem(p, nj)
        rs = ring(p, RS)
        k = "ABCDE".index(kind)
        q = me if kind in "AB" else qx
        dev = {"A": partner, "B": x_dev, "C": y_dev, "D": partner, "E": partner}[kind]
        if kind == "A":
            rows, rows_d = pl.ds(0, dq), pl.ds(0, 64)
        else:
            side = 1 - y if kind == "E" else y
            rows = pl.ds(pl.multiple_of(side * hq, 16), hq)
            rows_d = pl.ds(pl.multiple_of(side * 32, 32), 32)
        sems = w_snd.at[k, 0, rs], w_rcv.at[k, 0, rs]
        if kind in "AB" and not whole:
            for src, gu, lanes in shard_parts(l, t, rows):
                yield remote(src, ggu.at[p, q, gu, rows, lanes], *sems, dev)
        else:
            both = ggu.at[p, q, :, rows]
            yield remote(both, both, *sems, dev)
        wd_dst = gwd.at[p, q, rows_d]
        wd_src = wd_ref.at[l, t, rows_d] if kind in "AB" else wd_dst
        yield remote(wd_src, wd_dst, w_snd.at[k, 1, rs], w_rcv.at[k, 1, rs], dev)

    def pieces(span, act):
        def body(p, _):
            act(p)
            return 0

        lax.fori_loop(*span, body, 0)

    def weight_start(kinds, p):
        for kind in kinds:
            for cp in weight_copies(kind, p, False):
                cp.start()

    def weight_wait_recv(kinds, p):
        for kind in kinds:
            for cp in weight_copies(kind, p, True):
                cp.wait_recv()

    def weight_wait_send(kinds, p):
        for kind in kinds:
            for cp in weight_copies(kind, p, True):
                cp.wait_send()

    def weights_wait(sent):
        def arrived_x(p):
            weight_wait_recv("B", p)
            weight_wait_send("AB", p)

        def arrived_y(p):
            weight_wait_recv("C", p)
            weight_wait_send("CD", p)

        def complete(p):
            weight_wait_recv("ADE", p)
            weight_wait_send("E", p)

        pieces((sent[3], sent[2]), arrived_x)
        pieces((sent[5], sent[4]), arrived_y)
        pieces((sent[7], sent[6]), complete)

    def weights_send(sent):
        pieces((sent[1], sent[0]), functools.partial(weight_start, "BA"))
        pieces((sent[3], sent[2]), functools.partial(weight_start, "CD"))
        pieces((sent[5], sent[4]), functools.partial(weight_start, "E"))

    def weight_loads(s):
        slot = ring(s, 3)
        l, t = layer_of(s), rem(s, nj)

        def copy(src, dst, i):
            return pltpu.make_async_copy(src, dst, wl_sem.at[slot, i])

        for d in range(4):
            q = rem(me + d, 4)
            rows = pl.ds(pl.multiple_of(q * dq, 16), dq)
            if d == 0:
                for src, gu, lanes in shard_parts(l, t, pl.ds(0, dq)):
                    yield True, copy(src, wgu_b.at[slot, gu, rows, lanes], 0)
            else:
                yield True, copy(ggu.at[s, q], wgu_b.at[slot, :, rows], 0)
        for e in range(2):
            core, piece = owner_piece(t, e)
            for xx in range(2):
                q = xx * 2 + core
                dst = wd_b.at[slot, pl.ds(xx * 128 + e * 64, 64)]
                yield q == me, copy(wd_ref.at[l, piece], dst, 1)
                yield q != me, copy(gwd.at[s - t + piece, q], dst, 1)

    def load_start(s, cond):
        for mine, cp in weight_loads(s):
            start_if(cond & mine, [cp])

    def load_wait(s):
        slot = ring(s, 3)
        for i, buf in enumerate((wgu_b, wd_b)):
            pltpu.make_async_copy(buf.at[slot], buf.at[slot], wl_sem.at[slot, i]).wait()

    def core_copies(b):
        r, a, z = ring(b, 8), ring(b, 2), ring(b, 2)
        return (
            remote(sg.at[a, :, :, 1 - c], rdg.at[z], d_snd.at[0, r], d_rcv.at[0, r], partner),
            remote(sd.at[a, :, 1 - c], rdd.at[z], d_snd.at[1, r], d_rcv.at[1, r], partner),
        )

    def x_copies(b):
        r, a, z = ring(b, 8), ring(b, 2), ring(b, 4)
        return (
            remote(xsg.at[a], rxg.at[z], x_snd.at[0, r], x_rcv.at[0, r], x_dev),
            remote(xsd.at[a], rxd.at[z], x_snd.at[1, r], x_rcv.at[1, r], x_dev),
        )

    def y_copies(b):
        r, a, z = ring(b, 8), ring(b, 2), ring(b, 4)
        return (
            remote(ysg.at[a], ryg.at[z], y_snd.at[0, r], y_rcv.at[0, r], y_dev),
            remote(ysd.at[a], ryd.at[z], y_snd.at[1, r], y_rcv.at[1, r], y_dev),
        )

    def valid(b):
        return (b >= 0) & (b < steps)

    def start_if(cond, copies):
        for cp in copies:
            @pl.when(cond)
            def _():
                cp.start()

    def start_all(copies, b, cond=None):
        start_if(valid(b) if cond is None else valid(b) & cond, copies(b))

    def wait_all(copies, b):
        @pl.when(valid(b))
        def _():
            for cp in copies(b):
                cp.wait_recv()
            for cp in copies(b):
                cp.wait_send()

    def out_gate_up(b):
        a = ring(b, 2)
        l, m = layer_of(b), block_of(rem(b, nj))
        cps = []
        for gu, out in enumerate((dg_ref, du_ref)):
            for hf in range(2):
                cols = pl.ds(pl.multiple_of(hf * half + m * 128, 128), 128)
                src = fog.at[a, gu, :, pl.ds(hf * 128, 128)]
                cps.append(pltpu.make_async_copy(src, out.at[l, :, cols], o_sem.at[gu * 2 + hf, a]))
        return cps

    def out_down(b, own):
        a, r = ring(b, 2), ring(b, 8)
        core, piece = owner_piece(rem(b, nj), c)
        dst = dd_ref.at[layer_of(b), pl.ds(pl.multiple_of(piece * 64, 64), 64)]
        if own:
            return pltpu.make_async_copy(fod.at[a], dst, f_loc.at[a])
        return remote(fod.at[a], dst, f_snd.at[r], f_rcv.at[r], partner)

    def out_start(b, cond=None):
        ok = valid(b) if cond is None else valid(b) & cond
        core, _ = owner_piece(rem(b + BASE * nj, nj), c)

        start_if(ok, out_gate_up(b))
        start_if(ok & (core == c), [out_down(b, True)])
        start_if(ok & (core != c), [out_down(b, False)])

    def out_wait(b):
        @pl.when(valid(b))
        def _():
            for cp in out_gate_up(b):
                cp.wait()
            core, _ = owner_piece(rem(b, nj), c)
            theirs, _ = owner_piece(rem(b, nj), 1 - c)

            @pl.when(core == c)
            def _():
                out_down(b, True).wait()

            @pl.when(core != c)
            def _():
                out_down(b, False).wait_send()

            @pl.when(theirs == c)
            def _():
                out_down(b, False).wait_recv()

    def sum_y(b):
        a, z = ring(b, 2), ring(b, 4)
        for i in range(2):
            fog[a, i] = ysg[a, i] + ryg[z, i]
        fod[a] = ysd[a] + ryd[z]

    def sum_x(b):
        a, z = ring(b, 2), ring(b, 4)
        for i in range(2):
            ysg[a, i] = pog[a, i] + rxg[z, i]
        ysd[a] = pod[a] + rxd[z]

    def sum_cores(b):
        a = ring(b, 2)
        for i in range(2):
            pog[a, i] = sg[a, i, x, c] + rdg[a, i, x]
            xsg[a, i] = sg[a, i, 1 - x, c] + rdg[a, i, 1 - x]
        pod[a] = sd[a, x, c] + rdd[a, x]
        xsd[a] = sd[a, 1 - x, c] + rdd[a, 1 - x]

    def ahead(s):
        return (s > steps - SHORT).astype(jnp.int32)

    def front(s, sent):
        sent = (next_piece(s + LEAD, sent[0]), *sent[:-1])

        @pl.when((s + 1 >= 0) & (s + 1 < steps))
        def _():
            load_wait(s + 1)

        k = ahead(s)
        wait_all(core_copies, s - 2)
        wait_all(x_copies, s - 4 + k)
        wait_all(y_copies, s - 6 + k)
        out_wait(s - 8 + k)

        full = (s >= 6) & (s < steps - SHORT)

        @pl.when(full)
        def _():
            sum_y(s - 6)
            sum_x(s - 4)
            sum_cores(s - 2)

        for f, b in ((sum_y, s - 6 + k), (sum_x, s - 4 + k)):
            @pl.when(valid(b) & ((s < 6) | (s >= steps - SHORT)))
            def _():
                f(b)

        @pl.when(s == steps - SHORT)
        def _():
            wait_all(x_copies, s - 3)
            wait_all(y_copies, s - 5)
            out_wait(s - 7)
            sum_y(s - 5)
            sum_x(s - 3)

        @pl.when(valid(s - 2) & ((s < 6) | (s >= steps - SHORT)))
        def _():
            sum_cores(s - 2)

        @pl.when(s < LEAD)
        def _():
            weights_wait(sent)

        for i, recv, send in ((2, "B", "AB"), (4, "C", "CD"), (6, "ADE", "E")):
            @pl.when((s >= LEAD) & (sent[i] > sent[i + 1]))
            def _():
                weight_wait_recv(recv, sent[i + 1])
                weight_wait_send(send, sent[i + 1])

        return sent

    def starts(s, sent, cond=None):
        k = ahead(s)

        def also(c):
            return c if cond is None else c & cond

        if cond is None:
            weights_send(sent)
        else:
            for i, kinds in ((0, "BA"), (2, "CD"), (4, "E")):
                for kind in kinds:
                    start_if(also(sent[i] > sent[i + 1]), weight_copies(kind, sent[i + 1], False))

        start_all(core_copies, s - 1, cond)
        start_all(x_copies, s - 2, cond)
        start_all(y_copies, s - 4 + k, cond)
        out_start(s - 6 + k, cond)

        load_start(s + 2, also(valid(s + 2)))
        last = s == steps - SHORT
        start_all(y_copies, s - 3, also(last))
        out_start(s - 5, also(last))

    def boundary(s, sent):
        sent = front(s, sent)
        starts(s, sent)
        return sent

    blocks = tokens // tb

    def prepare(s):
        for i in range(2):
            hb[0, i] = wgu_b[ring(s, 3), i].T

    def first(s, t):
        tok = pl.ds(t * tb, tb)
        u = dot(hb[0, 0], n_t[:, tok])
        v = dot(hb[0, 1], n_t[:, tok])
        da = dot(wd_b[ring(s, 3)], gb_t[:, tok])
        sig = jax.nn.sigmoid(u)
        silu = u * sig
        s_a[t % 2] = (silu * v).astype(BF16)
        s_du[t % 2] = (da * v * sig * (1.0 + u * (1.0 - sig))).astype(BF16)
        s_dv[t % 2] = (da * silu).astype(BF16)

    def second(s, t):
        tok = pl.ds(t * tb, tb)
        slot, w = ring(s, 2), ring(s, 3)
        for i, val in enumerate((s_du, s_dv)):
            part = dot_nt(n_t[:, tok], val[t % 2])
            if t > 0:
                part = acc[i] + part
            if t < blocks - 1:
                acc[i] = part
            else:
                sg[slot, i] = part.reshape(2, 2, dq, FB)
        part = dot_nt(gb_t[:, tok], s_a[t % 2])
        if t > 0:
            part = acc[2] + part
        if t < blocks - 1:
            acc[2] = part
        else:
            sd[slot] = part.T.reshape(2, 2, 64, width)
        dn_t[:, tok] += dot(wgu_b[w, 0], s_du[t % 2]) + dot(wgu_b[w, 1], s_dv[t % 2])

    def compute(s):
        for t in range(1, blocks):
            first(s, t)
            second(s, t - 1)
        prepare(s + 1)
        first(s + 1, 0)
        second(s, blocks - 1)

    n_tok = tokens // nb

    def tok_of(i):
        return pl.ds(pl.multiple_of(i * nb, nb), nb)

    def rows_load(i, src, which):
        return pltpu.make_async_copy(src.at[tok_of(i)], hb.at[ring(i, 2), which], hb_sem.at[ring(i, 2), which])

    def g_load(i):
        return pltpu.make_async_copy(gt_ref.at[:, tok_of(i)], acc.at[ring(i, 3)], gl_sem.at[ring(i, 3)])

    def g_store(i):
        return pltpu.make_async_copy(acc.at[ring(i, 3)], gt_ref.at[:, tok_of(i)], gs_sem.at[ring(i, 3)])

    groups = [pl.ds(k, 128) for k in range(0, width, 128)]

    def new_norm(i):
        tok = tok_of(i)
        total = jnp.zeros((1, nb), F32)
        for rows in groups:
            xt = hb[ring(i, 2), 1, :, rows].T
            n_t[rows, tok] = xt
            xf = xt.astype(F32)
            total += jnp.sum(xf * xf, axis=0, keepdims=True)
        r = lax.rsqrt(total * (1.0 / width) + EPS)
        r_row[:, tok] = r
        for rows in groups:
            n_t[rows, tok] = (n_t[rows, tok].astype(F32) * r).astype(BF16)
            dn_t[rows, tok] = jnp.zeros((128, nb), F32)

    def new_g(i, put):
        tok = tok_of(i)
        r = r_row[:, tok]
        total = jnp.zeros((1, nb), F32)
        for rows in groups:
            xt = hb[ring(i, 2), 0, :, rows].T
            gb_t[rows, tok] = xt
            total += jnp.sum(dn_t[rows, tok] * (xt.astype(F32) * r), axis=0, keepdims=True)
        m = total * (1.0 / width)
        for rows in groups:
            nf = gb_t[rows, tok].astype(F32) * r
            put(rows, acc[ring(i, 3), rows] + r * (dn_t[rows, tok] - nf * m))

    def enter_block(i):
        h_new = h_ref.at[layers - 1]

        @pl.when(i == 0)
        def _():
            rows_load(i, g_ref, 0).start()
            rows_load(i, h_new, 1).start()

        @pl.when(i + 1 < n_tok)
        def _():
            rows_load(i + 1, g_ref, 0).start()
            rows_load(i + 1, h_new, 1).start()

        @pl.when(i >= 3)
        def _():
            g_store(i - 3).wait()

        rows_load(i, g_ref, 0).wait()
        rows_load(i, h_new, 1).wait()
        for rows in groups:
            gb = hb[ring(i, 2), 0, :, rows].T
            gb_t[rows, tok_of(i)] = gb
            acc[ring(i, 3), rows] = gb.astype(F32)
        new_norm(i)
        g_store(i).start()

    def stores_done():
        for i in range(n_tok - 3, n_tok):
            g_store(i).wait()

    def between(l_new):
        h_old, h_new = h_ref.at[l_new + 1], h_ref.at[l_new]
        rows_load(0, h_old, 0).start()
        rows_load(0, h_new, 1).start()
        g_load(0).start()

        def body(i, _):
            @pl.when(i >= 2)
            def _():
                g_store(i - 2).wait()

            @pl.when(i + 1 < n_tok)
            def _():
                rows_load(i + 1, h_old, 0).start()
                rows_load(i + 1, h_new, 1).start()
                g_load(i + 1).start()

            rows_load(i, h_old, 0).wait()
            rows_load(i, h_new, 1).wait()
            g_load(i).wait()

            def put(rows, g):
                acc[ring(i, 3), rows] = g
                gb_t[rows, tok_of(i)] = g.astype(BF16)

            new_g(i, put)
            new_norm(i)
            g_store(i).start()
            return 0

        lax.fori_loop(0, n_tok, body, 0)
        for i in range(n_tok - 2, n_tok):
            g_store(i).wait()

    def leave():
        h_old = h_ref.at[0]

        def dh_store(i):
            return pltpu.make_async_copy(hb.at[ring(i, 2), 1], dh_ref.at[tok_of(i)], do_sem.at[ring(i, 2)])

        rows_load(0, h_old, 0).start()
        g_load(0).start()

        def body(i, _):
            @pl.when(i + 1 < n_tok)
            def _():
                rows_load(i + 1, h_old, 0).start()
                g_load(i + 1).start()

            @pl.when(i >= 2)
            def _():
                dh_store(i - 2).wait()

            rows_load(i, h_old, 0).wait()
            g_load(i).wait()

            def put(rows, g):
                hb[ring(i, 2), 1, :, rows] = g.astype(BF16).T

            new_g(i, put)
            dh_store(i).start()
            return 0

        lax.fori_loop(0, n_tok, body, 0)
        for i in range(n_tok - 2, n_tok):
            dh_store(i).wait()

    barrier = pltpu.get_barrier_semaphore()
    for dev in (partner, x_dev, y_dev):
        pl.semaphore_signal(barrier, inc=1, device_id=dev, device_id_type=MESH)
    pl.semaphore_wait(barrier, 3)

    per = n_tok // (LEAD - 1)

    def lead_in(i, sent):
        sent = boundary(i - LEAD, sent)

        @pl.when(i < LEAD - 1)
        def _():
            for k in range(per):
                enter_block(i * per + k)

        return sent

    sent = lax.fori_loop(0, LEAD, lead_in, (jnp.int32(0),) * 8)
    stores_done()

    def main(s, sent):
        sent = front(s, sent)
        apart = (rem(s, nj) == 0) | (s < LEAD)

        @pl.when(apart)
        def _():
            starts(s, sent)

        @pl.when(rem(s, nj) == 0)
        def _():
            @pl.when(s > 0)
            def _():
                between(layer_of(s))

            prepare(s)
            first(s, 0)

        starts(s, sent, jnp.logical_not(apart))
        compute(s)
        return sent

    sent = lax.fori_loop(0, steps, main, sent)
    sent = lax.fori_loop(steps, steps + 2, boundary, sent)
    leave()
    lax.fori_loop(steps + 2, steps + 7, boundary, sent)


def backward(dims, h, g, gate, up, wd):
    layers, tokens, width, hidden, tb, nb = dims
    dq = width // 4
    nj = hidden // FB
    steps = layers * nj
    dma = pltpu.SemaphoreType.DMA
    vm = pltpu.VMEM
    anyspace = pl.BlockSpec(memory_space=pl.ANY)
    sds = jax.ShapeDtypeStruct
    out_shape = [
        sds((layers, dq, hidden), F32),
        sds((layers, dq, hidden), F32),
        sds((layers, hidden // 4, width), F32),
        sds((tokens, width), BF16),
        sds((steps, 4, 2, dq, FB), BF16),
        sds((steps, 4, 64, width), BF16),
        sds((width, tokens), F32),
    ]

    def pair(n):
        return [vm((n, 2, dq, FB), F32), vm((n, 64, width), F32)]

    scratch = [
        vm((width, tokens), BF16),
        vm((width, tokens), BF16),
        vm((width, tokens), F32),
        vm((1, tokens), F32),
        vm((3, 2, width, FB), BF16),
        vm((3, FB, width), BF16),
        vm((2, FB, tb), BF16),
        vm((2, FB, tb), BF16),
        vm((2, FB, tb), BF16),
        vm((3, width, FB), F32),
        vm((2, 2, nb, width), BF16),
        vm((2, 2, 2, 2, dq, FB), F32),
        vm((2, 2, 2, 64, width), F32),
        vm((2, 2, 2, dq, FB), F32),
        vm((2, 2, 64, width), F32),
        *pair(2), *pair(2), *pair(4), *pair(2), *pair(4), *pair(2),
        dma((3, 2)),
        dma((2, 8)), dma((2, 8)), dma((2, 8)), dma((2, 8)), dma((2, 8)), dma((2, 8)),
        dma((4, 2)), dma((2,)), dma((8,)), dma((8,)),
        dma((5, 2, RS)), dma((5, 2, RS)),
        dma((2, 2)), dma((3,)), dma((3,)), dma((2,)),
    ]
    return pl.pallas_call(
        functools.partial(kernel, dims),
        out_shape=out_shape,
        in_specs=[anyspace] * 5,
        out_specs=[anyspace] * 7,
        scratch_shapes=scratch,
        compiler_params=pltpu.CompilerParams(
            collective_id=0, has_side_effects=True, vmem_limit_bytes=67043328,
        ),
        name="mlp_backward",
    )(h, g, gate, up, wd)[:4]


def solution(mesh):
    tok_spec = P(("dp", "fsdp"))
    stack_spec = P(None, ("dp", "fsdp"))
    weight_spec = P(None, "fsdp")

    def local_backward(h_saved, grad_out, gate_sh, up_sh, down_sh):
        layers = h_saved.shape[0]
        b_loc, seq, width = grad_out.shape
        tokens = b_loc * seq
        dq, hidden = gate_sh.shape[1:]
        nj = hidden // FB
        tb = min(512, tokens // 2)
        nb = FB
        wd = down_sh.reshape(layers, nj, 64, width)
        dims = (layers, tokens, width, hidden, tb, nb)
        d_gate, d_up, d_down, d_h0 = backward(
            dims, h_saved.reshape(layers, tokens, width), grad_out.reshape(tokens, width), gate_sh, up_sh, wd
        )
        return d_gate, d_up, d_down, d_h0.reshape(b_loc, seq, width)

    return jax.shard_map(
        local_backward,
        mesh=mesh,
        in_specs=(stack_spec, tok_spec, weight_spec, weight_spec, weight_spec),
        out_specs=(weight_spec, weight_spec, weight_spec, tok_spec),
        check_vma=False,
    )
```

```python
import functools

import jax
import jax.numpy as jnp
from jax import lax
from jax.experimental import pallas as pl
from jax.experimental.pallas import tpu as pltpu
from jax.sharding import PartitionSpec as P

EPS = 1e-5
MESH = pl.DeviceIdType.MESH
F32 = jnp.float32
BF16 = jnp.bfloat16
FB = 256
LEAD = 8
BURST = 5
RS = 32
SHORT = 4
BASE = 240
DOT_NT = (((1,), (1,)), ((), ()))


def div(a, b):
    return a // b if isinstance(a, int) else lax.div(a, jnp.int32(b))


def rem(a, b):
    return a % b if isinstance(a, int) else lax.rem(a, jnp.int32(b))


def ring(i, n):
    return rem(i + BASE, n)


def dot(a, b):
    return jnp.dot(a, b, preferred_element_type=F32)


def dot_nt(a, b):
    return lax.dot_general(a, b, DOT_NT, preferred_element_type=F32)


def kernel(
    dims, h_ref, g_ref, gate_ref, up_ref, wd_ref,
    dgu_ref, dd_ref, dh_ref, ggu, gwd, gt_ref,
    n_t, gb_t, dn_t, r_row, wgu_b, wd_b, s_a, s_du, s_dv, acc, hb,
    sg, sd, rdg, rdd, xsg, xsd, pog, pod, rxg, rxd, ysg, ysd, ryg, ryd, fog, fod,
    wl_sem, d_snd, d_rcv, x_snd, x_rcv, y_snd, y_rcv, o_sem, f_loc, f_snd, f_rcv,
    w_snd, w_rcv, hb_sem, gl_sem, gs_sem, do_sem,
):
    layers, tokens, width, hidden, tb, nb = dims
    dq = width // 4
    hq = dq // 2
    half = hidden // 2
    nj = hidden // FB
    mid = nj // 2
    steps = layers * nj
    y = lax.axis_index("dp")
    me = lax.axis_index("fsdp")
    x = me // 2
    c = me % 2
    qx = (1 - x) * 2 + c
    partner = (y, x * 2 + 1 - c)
    x_dev = (y, qx)
    y_dev = (1 - y, me)

    def layer_of(s):
        return layers - 1 - div(s, nj)

    def block_of(t):
        return div(t, 2) + rem(t, 2) * (mid + 1)

    def owner_piece(t, e):
        last = div(t, nj - 1)
        core = (1 - last) * rem(t, 2) + last * e
        piece = (1 - last) * (t + e) + last * (nj - 1) * (1 - e)
        return core, piece

    def remote(src, dst, snd, rcv, dev):
        return pltpu.make_async_remote_copy(
            src_ref=src, dst_ref=dst, send_sem=snd, recv_sem=rcv, device_id=dev, device_id_type=MESH
        )

    def next_piece(beta, n):
        burst = ((beta >= LEAD) & (beta < LEAD + 2)).astype(jnp.int32)
        skip = ((beta >= LEAD + 2) & (rem(beta, 9) == 4)).astype(jnp.int32)
        return n + (1 + (BURST - 1) * burst - skip) * (n < steps).astype(jnp.int32)

    def shard_parts(l, t, rows):
        m = block_of(t)
        for gu, ref in enumerate((gate_ref, up_ref)):
            for hf in range(2):
                cols = pl.ds(pl.multiple_of(hf * half + m * 128, 128), 128)
                yield ref.at[l, rows, cols], gu, pl.ds(hf * 128, 128)

    def weight_copies(kind, p, whole):
        l, t = layer_of(p), rem(p, nj)
        rs = ring(p, RS)
        k = "ABCDE".index(kind)
        q = me if kind in "AB" else qx
        dev = {"A": partner, "B": x_dev, "C": y_dev, "D": partner, "E": partner}[kind]
        if kind == "A":
            rows, rows_d = pl.ds(0, dq), pl.ds(0, 64)
        else:
            side = 1 - y if kind == "E" else y
            rows = pl.ds(pl.multiple_of(side * hq, 16), hq)
            rows_d = pl.ds(pl.multiple_of(side * 32, 32), 32)
        sems = w_snd.at[k, 0, rs], w_rcv.at[k, 0, rs]
        if kind in "AB" and not whole:
            for src, gu, lanes in shard_parts(l, t, rows):
                yield remote(src, ggu.at[p, q, gu, rows, lanes], *sems, dev)
        else:
            both = ggu.at[p, q, :, rows]
            yield remote(both, both, *sems, dev)
        wd_dst = gwd.at[p, q, rows_d]
        wd_src = wd_ref.at[l, t, rows_d] if kind in "AB" else wd_dst
        yield remote(wd_src, wd_dst, w_snd.at[k, 1, rs], w_rcv.at[k, 1, rs], dev)

    def pieces(span, act):
        def body(p, _):
            act(p)
            return 0

        lax.fori_loop(*span, body, 0)

    def weight_start(kinds, p):
        for kind in kinds:
            for cp in weight_copies(kind, p, False):
                cp.start()

    def weight_wait_recv(kinds, p):
        for kind in kinds:
            for cp in weight_copies(kind, p, True):
                cp.wait_recv()

    def weight_wait_send(kinds, p):
        for kind in kinds:
            for cp in weight_copies(kind, p, True):
                cp.wait_send()

    def weights_wait(sent):
        def arrived_x(p):
            weight_wait_recv("B", p)
            weight_wait_send("AB", p)

        def arrived_y(p):
            weight_wait_recv("C", p)
            weight_wait_send("CD", p)

        def complete(p):
            weight_wait_recv("ADE", p)
            weight_wait_send("E", p)

        pieces((sent[3], sent[2]), arrived_x)
        pieces((sent[5], sent[4]), arrived_y)
        pieces((sent[6], sent[5]), complete)

    def weights_send(sent):
        pieces((sent[1], sent[0]), functools.partial(weight_start, "BA"))
        pieces((sent[3], sent[2]), functools.partial(weight_start, "CD"))
        pieces((sent[5], sent[4]), functools.partial(weight_start, "E"))

    def weight_loads(s):
        slot = ring(s, 3)
        l, t = layer_of(s), rem(s, nj)

        def copy(src, dst, i):
            return pltpu.make_async_copy(src, dst, wl_sem.at[slot, i])

        for d in range(4):
            q = rem(me + d, 4)
            rows = pl.ds(pl.multiple_of(q * dq, 16), dq)
            if d == 0:
                for src, gu, lanes in shard_parts(l, t, pl.ds(0, dq)):
                    yield True, copy(src, wgu_b.at[slot, gu, rows, lanes], 0)
            else:
                yield True, copy(ggu.at[s, q], wgu_b.at[slot, :, rows], 0)
        for e in range(2):
            core, piece = owner_piece(t, e)
            for xx in range(2):
                q = xx * 2 + core
                dst = wd_b.at[slot, pl.ds(xx * 128 + e * 64, 64)]
                yield q == me, copy(wd_ref.at[l, piece], dst, 1)
                yield q != me, copy(gwd.at[s - t + piece, q], dst, 1)

    def load_start(s, cond):
        for mine, cp in weight_loads(s):
            start_if(cond & mine, [cp])

    def load_wait(s):
        slot = ring(s, 3)
        for i, buf in enumerate((wgu_b, wd_b)):
            pltpu.make_async_copy(buf.at[slot], buf.at[slot], wl_sem.at[slot, i]).wait()

    def core_copies(b):
        r, a, z = ring(b, 8), ring(b, 2), ring(b, 2)
        return (
            remote(sg.at[a, :, :, 1 - c], rdg.at[z], d_snd.at[0, r], d_rcv.at[0, r], partner),
            remote(sd.at[a, :, 1 - c], rdd.at[z], d_snd.at[1, r], d_rcv.at[1, r], partner),
        )

    def x_copies(b):
        r, a, z = ring(b, 8), ring(b, 2), ring(b, 4)
        return (
            remote(xsg.at[a], rxg.at[z], x_snd.at[0, r], x_rcv.at[0, r], x_dev),
            remote(xsd.at[a], rxd.at[z], x_snd.at[1, r], x_rcv.at[1, r], x_dev),
        )

    def y_copies(b):
        r, a, z = ring(b, 8), ring(b, 2), ring(b, 4)
        return (
            remote(ysg.at[a], ryg.at[z], y_snd.at[0, r], y_rcv.at[0, r], y_dev),
            remote(ysd.at[a], ryd.at[z], y_snd.at[1, r], y_rcv.at[1, r], y_dev),
        )

    def valid(b):
        return (b >= 0) & (b < steps)

    def start_if(cond, copies):
        for cp in copies:
            @pl.when(cond)
            def _():
                cp.start()

    def start_all(copies, b, cond=None):
        start_if(valid(b) if cond is None else valid(b) & cond, copies(b))

    def wait_all(copies, b):
        @pl.when(valid(b))
        def _():
            for cp in copies(b):
                cp.wait_recv()
            for cp in copies(b):
                cp.wait_send()

    def out_gate_up(b):
        a = ring(b, 2)
        l, m = layer_of(b), block_of(rem(b, nj))
        for hf in range(2):
            cols = pl.ds(pl.multiple_of(hf * half + m * 128, 128), 128)
            yield pltpu.make_async_copy(fog.at[a, :, :, pl.ds(hf * 128, 128)], dgu_ref.at[:, l, :, cols], o_sem.at[a])

    def out_down(b, own):
        a, r = ring(b, 2), ring(b, 8)
        core, piece = owner_piece(rem(b, nj), c)
        dst = dd_ref.at[layer_of(b), pl.ds(pl.multiple_of(piece * 64, 64), 64)]
        if own:
            return pltpu.make_async_copy(fod.at[a], dst, f_loc.at[a])
        return remote(fod.at[a], dst, f_snd.at[r], f_rcv.at[r], partner)

    def out_start(b, cond=None):
        ok = valid(b) if cond is None else valid(b) & cond
        core, _ = owner_piece(rem(b + BASE * nj, nj), c)

        start_if(ok, out_gate_up(b))
        start_if(ok & (core == c), [out_down(b, True)])
        start_if(ok & (core != c), [out_down(b, False)])

    def out_wait(b):
        @pl.when(valid(b))
        def _():
            a = ring(b, 2)
            pltpu.make_async_copy(fog.at[a], fog.at[a], o_sem.at[a]).wait()
            core, _ = owner_piece(rem(b, nj), c)
            theirs, _ = owner_piece(rem(b, nj), 1 - c)

            @pl.when(core == c)
            def _():
                out_down(b, True).wait()

            @pl.when(core != c)
            def _():
                out_down(b, False).wait_send()

            @pl.when(theirs == c)
            def _():
                out_down(b, False).wait_recv()

    def sum_y(b):
        a, z = ring(b, 2), ring(b, 4)
        for i in range(2):
            fog[a, i] = ysg[a, i] + ryg[z, i]
        fod[a] = ysd[a] + ryd[z]

    def sum_x(b):
        a, z = ring(b, 2), ring(b, 4)
        for i in range(2):
            ysg[a, i] = pog[a, i] + rxg[z, i]
        ysd[a] = pod[a] + rxd[z]

    def sum_cores(b):
        a = ring(b, 2)
        for i in range(2):
            pog[a, i] = sg[a, i, x, c] + rdg[a, i, x]
            xsg[a, i] = sg[a, i, 1 - x, c] + rdg[a, i, 1 - x]
        pod[a] = sd[a, x, c] + rdd[a, x]
        xsd[a] = sd[a, 1 - x, c] + rdd[a, 1 - x]

    def ahead(s):
        return (s > steps - SHORT).astype(jnp.int32)

    def front(s, sent):
        sent = (next_piece(s + LEAD, sent[0]), *sent[:-1])

        @pl.when((s + 1 >= 0) & (s + 1 < steps))
        def _():
            load_wait(s + 1)

        k = ahead(s)
        wait_all(core_copies, s - 2)
        wait_all(x_copies, s - 4 + k)
        wait_all(y_copies, s - 6 + k)
        out_wait(s - 8 + k)

        full = (s >= 6) & (s < steps - SHORT)

        @pl.when(full)
        def _():
            sum_y(s - 6)
            sum_x(s - 4)
            sum_cores(s - 2)

        for f, b in ((sum_y, s - 6 + k), (sum_x, s - 4 + k)):
            @pl.when(valid(b) & ((s < 6) | (s >= steps - SHORT)))
            def _():
                f(b)

        @pl.when(s == steps - SHORT)
        def _():
            wait_all(x_copies, s - 3)
            wait_all(y_copies, s - 5)
            out_wait(s - 7)
            sum_y(s - 5)
            sum_x(s - 3)

        @pl.when(valid(s - 2) & ((s < 6) | (s >= steps - SHORT)))
        def _():
            sum_cores(s - 2)

        @pl.when(s < LEAD)
        def _():
            weights_wait(sent)

        for i, recv, send in ((2, "B", "AB"), (4, "C", "CD"), (5, "ADE", "E")):
            @pl.when((s >= LEAD) & (sent[i] > sent[i + 1]))
            def _():
                weight_wait_recv(recv, sent[i + 1])
                weight_wait_send(send, sent[i + 1])

        return sent

    def starts(s, sent, cond=None):
        k = ahead(s)

        def also(c):
            return c if cond is None else c & cond

        if cond is None:
            weights_send(sent)
        else:
            for i, kinds in ((0, "BA"), (2, "CD"), (4, "E")):
                for kind in kinds:
                    start_if(also(sent[i] > sent[i + 1]), weight_copies(kind, sent[i + 1], False))

        start_all(core_copies, s - 1, cond)
        start_all(x_copies, s - 2, cond)
        start_all(y_copies, s - 4 + k, cond)
        out_start(s - 6 + k, cond)

        load_start(s + 2, also(valid(s + 2)))
        last = s == steps - SHORT
        start_all(y_copies, s - 3, also(last))
        out_start(s - 5, also(last))

    def boundary(s, sent):
        sent = front(s, sent)
        starts(s, sent)
        return sent

    blocks = tokens // tb

    def prepare(s):
        for i in range(2):
            hb[0, i] = wgu_b[ring(s, 3), i].T

    def first(s, t):
        tok = pl.ds(t * tb, tb)
        u = dot(hb[0, 0], n_t[:, tok])
        v = dot(hb[0, 1], n_t[:, tok])
        da = dot(wd_b[ring(s, 3)], gb_t[:, tok])
        sig = jax.nn.sigmoid(u)
        silu = u * sig
        s_a[t % 2] = (silu * v).astype(BF16)
        s_du[t % 2] = (da * v * sig * (1.0 + u * (1.0 - sig))).astype(BF16)
        s_dv[t % 2] = (da * silu).astype(BF16)

    def second(s, t):
        tok = pl.ds(t * tb, tb)
        slot, w = ring(s, 2), ring(s, 3)
        for i, val in enumerate((s_du, s_dv)):
            part = dot_nt(n_t[:, tok], val[t % 2])
            if t > 0:
                part = acc[i] + part
            if t < blocks - 1:
                acc[i] = part
            else:
                sg[slot, i] = part.reshape(2, 2, dq, FB)
        part = dot_nt(gb_t[:, tok], s_a[t % 2])
        if t > 0:
            part = acc[2] + part
        if t < blocks - 1:
            acc[2] = part
        else:
            sd[slot] = part.T.reshape(2, 2, 64, width)
        dn_t[:, tok] += dot(wgu_b[w, 0], s_du[t % 2]) + dot(wgu_b[w, 1], s_dv[t % 2])

    def compute(s):
        for t in range(1, blocks):
            first(s, t)
            second(s, t - 1)
        prepare(s + 1)
        first(s + 1, 0)
        second(s, blocks - 1)

    n_tok = tokens // nb

    def tok_of(i):
        return pl.ds(pl.multiple_of(i * nb, nb), nb)

    def rows_load(i, src, which):
        return pltpu.make_async_copy(src.at[tok_of(i)], hb.at[ring(i, 2), which], hb_sem.at[ring(i, 2), which])

    def g_load(i):
        return pltpu.make_async_copy(gt_ref.at[:, tok_of(i)], acc.at[ring(i, 3)], gl_sem.at[ring(i, 3)])

    def g_store(i):
        return pltpu.make_async_copy(acc.at[ring(i, 3)], gt_ref.at[:, tok_of(i)], gs_sem.at[ring(i, 3)])

    groups = [pl.ds(k, 128) for k in range(0, width, 128)]

    def new_norm(i):
        tok = tok_of(i)
        total = jnp.zeros((1, nb), F32)
        for rows in groups:
            xt = hb[ring(i, 2), 1, :, rows].T
            n_t[rows, tok] = xt
            xf = xt.astype(F32)
            total += jnp.sum(xf * xf, axis=0, keepdims=True)
        r = lax.rsqrt(total * (1.0 / width) + EPS)
        r_row[:, tok] = r
        for rows in groups:
            n_t[rows, tok] = (n_t[rows, tok].astype(F32) * r).astype(BF16)
            dn_t[rows, tok] = jnp.zeros((128, nb), F32)

    def new_g(i, put):
        tok = tok_of(i)
        r = r_row[:, tok]
        total = jnp.zeros((1, nb), F32)
        for rows in groups:
            xt = hb[ring(i, 2), 0, :, rows].T
            gb_t[rows, tok] = xt
            total += jnp.sum(dn_t[rows, tok] * (xt.astype(F32) * r), axis=0, keepdims=True)
        m = total * (1.0 / width)
        for rows in groups:
            nf = gb_t[rows, tok].astype(F32) * r
            put(rows, acc[ring(i, 3), rows] + r * (dn_t[rows, tok] - nf * m))

    def enter_block(i):
        h_new = h_ref.at[layers - 1]

        @pl.when(i == 0)
        def _():
            rows_load(i, g_ref, 0).start()
            rows_load(i, h_new, 1).start()

        @pl.when(i + 1 < n_tok)
        def _():
            rows_load(i + 1, g_ref, 0).start()
            rows_load(i + 1, h_new, 1).start()

        @pl.when(i >= 3)
        def _():
            g_store(i - 3).wait()

        rows_load(i, g_ref, 0).wait()
        rows_load(i, h_new, 1).wait()
        for rows in groups:
            gb = hb[ring(i, 2), 0, :, rows].T
            gb_t[rows, tok_of(i)] = gb
            acc[ring(i, 3), rows] = gb.astype(F32)
        new_norm(i)
        g_store(i).start()

    def stores_done():
        for i in range(n_tok - 3, n_tok):
            g_store(i).wait()

    def between(l_new):
        h_old, h_new = h_ref.at[l_new + 1], h_ref.at[l_new]
        rows_load(0, h_old, 0).start()
        rows_load(0, h_new, 1).start()
        g_load(0).start()

        def body(i, _):
            @pl.when(i >= 2)
            def _():
                g_store(i - 2).wait()

            @pl.when(i + 1 < n_tok)
            def _():
                rows_load(i + 1, h_old, 0).start()
                rows_load(i + 1, h_new, 1).start()
                g_load(i + 1).start()

            rows_load(i, h_old, 0).wait()
            rows_load(i, h_new, 1).wait()
            g_load(i).wait()

            def put(rows, g):
                acc[ring(i, 3), rows] = g
                gb_t[rows, tok_of(i)] = g.astype(BF16)

            new_g(i, put)
            new_norm(i)
            g_store(i).start()
            return 0

        lax.fori_loop(0, n_tok, body, 0)
        for i in range(n_tok - 2, n_tok):
            g_store(i).wait()

    def leave():
        h_old = h_ref.at[0]

        def dh_store(i):
            return pltpu.make_async_copy(hb.at[ring(i, 2), 1], dh_ref.at[tok_of(i)], do_sem.at[ring(i, 2)])

        rows_load(0, h_old, 0).start()
        g_load(0).start()

        def body(i, _):
            @pl.when(i + 1 < n_tok)
            def _():
                rows_load(i + 1, h_old, 0).start()
                g_load(i + 1).start()

            @pl.when(i >= 2)
            def _():
                dh_store(i - 2).wait()

            rows_load(i, h_old, 0).wait()
            g_load(i).wait()

            def put(rows, g):
                hb[ring(i, 2), 1, :, rows] = g.astype(BF16).T

            new_g(i, put)
            dh_store(i).start()
            return 0

        lax.fori_loop(0, n_tok, body, 0)
        for i in range(n_tok - 2, n_tok):
            dh_store(i).wait()

    barrier = pltpu.get_barrier_semaphore()
    for dev in (partner, x_dev, y_dev):
        pl.semaphore_signal(barrier, inc=1, device_id=dev, device_id_type=MESH)
    pl.semaphore_wait(barrier, 3)

    per = n_tok // LEAD

    def lead_in(i, sent):
        sent = boundary(i - LEAD, sent)
        for k in range(per):
            enter_block(i * per + k)
        return sent

    sent = lax.fori_loop(0, LEAD, lead_in, (jnp.int32(0),) * 8)
    stores_done()

    def main(s, sent):
        sent = front(s, sent)
        apart = (rem(s, nj) == 0) | (s < LEAD)

        @pl.when(apart)
        def _():
            starts(s, sent)

        @pl.when(rem(s, nj) == 0)
        def _():
            @pl.when(s > 0)
            def _():
                between(layer_of(s))

            prepare(s)
            first(s, 0)

        starts(s, sent, jnp.logical_not(apart))
        compute(s)
        return sent

    sent = lax.fori_loop(0, steps, main, sent)
    sent = lax.fori_loop(steps, steps + 2, boundary, sent)
    leave()
    lax.fori_loop(steps + 2, steps + 7, boundary, sent)


def backward(dims, h, g, gate, up, wd):
    layers, tokens, width, hidden, tb, nb = dims
    dq = width // 4
    nj = hidden // FB
    steps = layers * nj
    dma = pltpu.SemaphoreType.DMA
    vm = pltpu.VMEM
    anyspace = pl.BlockSpec(memory_space=pl.ANY)
    sds = jax.ShapeDtypeStruct
    out_shape = [
        sds((2, layers, dq, hidden), F32),
        sds((layers, hidden // 4, width), F32),
        sds((tokens, width), BF16),
        sds((steps, 4, 2, dq, FB), BF16),
        sds((steps, 4, 64, width), BF16),
        sds((width, tokens), F32),
    ]

    def pair(n):
        return [vm((n, 2, dq, FB), F32), vm((n, 64, width), F32)]

    scratch = [
        vm((width, tokens), BF16),
        vm((width, tokens), BF16),
        vm((width, tokens), F32),
        vm((1, tokens), F32),
        vm((3, 2, width, FB), BF16),
        vm((3, FB, width), BF16),
        vm((2, FB, tb), BF16),
        vm((2, FB, tb), BF16),
        vm((2, FB, tb), BF16),
        vm((3, width, FB), F32),
        vm((2, 2, nb, width), BF16),
        vm((2, 2, 2, 2, dq, FB), F32),
        vm((2, 2, 2, 64, width), F32),
        vm((2, 2, 2, dq, FB), F32),
        vm((2, 2, 64, width), F32),
        *pair(2), *pair(2), *pair(4), *pair(2), *pair(4), *pair(2),
        dma((3, 2)),
        dma((2, 8)), dma((2, 8)), dma((2, 8)), dma((2, 8)), dma((2, 8)), dma((2, 8)),
        dma((2,)), dma((2,)), dma((8,)), dma((8,)),
        dma((5, 2, RS)), dma((5, 2, RS)),
        dma((2, 2)), dma((3,)), dma((3,)), dma((2,)),
    ]
    return pl.pallas_call(
        functools.partial(kernel, dims),
        out_shape=out_shape,
        in_specs=[anyspace] * 5,
        out_specs=[anyspace] * 6,
        scratch_shapes=scratch,
        compiler_params=pltpu.CompilerParams(
            collective_id=0, has_side_effects=True, vmem_limit_bytes=67043328,
        ),
        name="mlp_backward",
    )(h, g, gate, up, wd)[:3]


def solution(mesh):
    tok_spec = P(("dp", "fsdp"))
    stack_spec = P(None, ("dp", "fsdp"))
    weight_spec = P(None, "fsdp")

    def local_backward(h_saved, grad_out, gate_sh, up_sh, down_sh):
        layers = h_saved.shape[0]
        b_loc, seq, width = grad_out.shape
        tokens = b_loc * seq
        dq, hidden = gate_sh.shape[1:]
        nj = hidden // FB
        tb = min(512, tokens // 2)
        nb = FB
        wd = down_sh.reshape(layers, nj, 64, width)
        dims = (layers, tokens, width, hidden, tb, nb)
        d_gate_up, d_down, d_h0 = backward(
            dims, h_saved.reshape(layers, tokens, width), grad_out.reshape(tokens, width), gate_sh, up_sh, wd
        )
        return d_gate_up[0], d_gate_up[1], d_down, d_h0.reshape(b_loc, seq, width)

    return jax.shard_map(
        local_backward,
        mesh=mesh,
        in_specs=(stack_spec, tok_spec, weight_spec, weight_spec, weight_spec),
        out_specs=(weight_spec, weight_spec, weight_spec, tok_spec),
        check_vma=False,
    )
```

```python
import functools

import jax
import jax.numpy as jnp
from jax import lax
from jax.experimental import pallas as pl
from jax.experimental.pallas import tpu as pltpu
from jax.sharding import PartitionSpec as P

EPS = 1e-5
MESH = pl.DeviceIdType.MESH
F32 = jnp.float32
BF16 = jnp.bfloat16
FB = 256
LEAD = 8
BURST = 5
RS = 32
SHORT = 4
BASE = 240
DOT_NT = (((1,), (1,)), ((), ()))


def div(a, b):
    return a // b if isinstance(a, int) else lax.div(a, jnp.int32(b))


def rem(a, b):
    return a % b if isinstance(a, int) else lax.rem(a, jnp.int32(b))


def ring(i, n):
    return rem(i + BASE, n)


def dot(a, b):
    return jnp.dot(a, b, preferred_element_type=F32)


def dot_nt(a, b):
    return lax.dot_general(a, b, DOT_NT, preferred_element_type=F32)


def kernel(
    dims, h_ref, g_ref, gate_ref, up_ref, wd_ref,
    dg_ref, du_ref, dd_ref, dh_ref, ggu, gwd, gt_ref,
    n_t, gb_t, dn_t, r_row, wgu_b, wd_b, s_a, s_du, s_dv, acc, hb,
    sg, sd, rdg, rdd, xsg, xsd, pog, pod, rxg, rxd, ysg, ysd, ryg, ryd, fog, fod,
    wl_sem, d_snd, d_rcv, x_snd, x_rcv, y_snd, y_rcv, o_sem, f_loc, f_snd, f_rcv,
    w_snd, w_rcv, hb_sem, gl_sem, gs_sem, do_sem,
):
    layers, tokens, width, hidden, tb, nb = dims
    dq = width // 4
    hq = dq // 2
    half = hidden // 2
    nj = hidden // FB
    mid = nj // 2
    steps = layers * nj
    y = lax.axis_index("dp")
    me = lax.axis_index("fsdp")
    x = me // 2
    c = me % 2
    qx = (1 - x) * 2 + c
    partner = (y, x * 2 + 1 - c)
    x_dev = (y, qx)
    y_dev = (1 - y, me)

    def layer_of(s):
        return layers - 1 - div(s, nj)

    def block_of(t):
        return div(t, 2) + rem(t, 2) * (mid + 1)

    def owner_piece(t, e):
        last = div(t, nj - 1)
        core = (1 - last) * rem(t, 2) + last * e
        piece = (1 - last) * (t + e) + last * (nj - 1) * (1 - e)
        return core, piece

    def remote(src, dst, snd, rcv, dev):
        return pltpu.make_async_remote_copy(
            src_ref=src, dst_ref=dst, send_sem=snd, recv_sem=rcv, device_id=dev, device_id_type=MESH
        )

    def next_piece(beta, n):
        burst = ((beta >= LEAD) & (beta < LEAD + 2)).astype(jnp.int32)
        skip = ((beta >= LEAD + 2) & (rem(beta, 9) == 4)).astype(jnp.int32)
        return n + (1 + (BURST - 1) * burst - skip) * (n < steps).astype(jnp.int32)

    def shard_parts(l, t, rows):
        m = block_of(t)
        for gu, ref in enumerate((gate_ref, up_ref)):
            for hf in range(2):
                cols = pl.ds(pl.multiple_of(hf * half + m * 128, 128), 128)
                yield ref.at[l, rows, cols], gu, pl.ds(hf * 128, 128)

    def weight_copies(kind, p, whole):
        l, t = layer_of(p), rem(p, nj)
        rs = ring(p, RS)
        k = "ABCDE".index(kind)
        q = me if kind in "AB" else qx
        dev = {"A": partner, "B": x_dev, "C": y_dev, "D": partner, "E": partner}[kind]
        if kind == "A":
            rows, rows_d = pl.ds(0, dq), pl.ds(0, 64)
        else:
            side = 1 - y if kind == "E" else y
            rows = pl.ds(pl.multiple_of(side * hq, 16), hq)
            rows_d = pl.ds(pl.multiple_of(side * 32, 32), 32)
        sems = w_snd.at[k, 0, rs], w_rcv.at[k, 0, rs]
        if kind in "AB" and not whole:
            for src, gu, lanes in shard_parts(l, t, rows):
                yield remote(src, ggu.at[p, q, gu, rows, lanes], *sems, dev)
        else:
            both = ggu.at[p, q, :, rows]
            yield remote(both, both, *sems, dev)
        wd_dst = gwd.at[p, q, rows_d]
        wd_src = wd_ref.at[l, t, rows_d] if kind in "AB" else wd_dst
        yield remote(wd_src, wd_dst, w_snd.at[k, 1, rs], w_rcv.at[k, 1, rs], dev)

    def pieces(span, act):
        def body(p, _):
            act(p)
            return 0

        lax.fori_loop(*span, body, 0)

    def weight_start(kinds, p):
        for kind in kinds:
            for cp in weight_copies(kind, p, False):
                cp.start()

    def weight_wait_recv(kinds, p):
        for kind in kinds:
            for cp in weight_copies(kind, p, True):
                cp.wait_recv()

    def weight_wait_send(kinds, p):
        for kind in kinds:
            for cp in weight_copies(kind, p, True):
                cp.wait_send()

    def weights_wait(sent):
        def arrived_x(p):
            weight_wait_recv("B", p)
            weight_wait_send("AB", p)

        def arrived_y(p):
            weight_wait_recv("C", p)
            weight_wait_send("CD", p)

        def complete(p):
            weight_wait_recv("ADE", p)
            weight_wait_send("E", p)

        pieces((sent[3], sent[2]), arrived_x)
        pieces((sent[5], sent[4]), arrived_y)
        pieces((sent[6], sent[5]), complete)

    def weights_send(sent):
        pieces((sent[1], sent[0]), functools.partial(weight_start, "BA"))
        pieces((sent[3], sent[2]), functools.partial(weight_start, "CD"))
        pieces((sent[5], sent[4]), functools.partial(weight_start, "E"))

    def weight_loads(s):
        slot = ring(s, 3)
        l, t = layer_of(s), rem(s, nj)

        def copy(src, dst, i):
            return pltpu.make_async_copy(src, dst, wl_sem.at[slot, i])

        for d in range(4):
            q = rem(me + d, 4)
            rows = pl.ds(pl.multiple_of(q * dq, 16), dq)
            if d == 0:
                for src, gu, lanes in shard_parts(l, t, pl.ds(0, dq)):
                    yield True, copy(src, wgu_b.at[slot, gu, rows, lanes], 0)
            else:
                yield True, copy(ggu.at[s, q], wgu_b.at[slot, :, rows], 0)
        for e in range(2):
            core, piece = owner_piece(t, e)
            for xx in range(2):
                q = xx * 2 + core
                dst = wd_b.at[slot, pl.ds(xx * 128 + e * 64, 64)]
                yield q == me, copy(wd_ref.at[l, piece], dst, 1)
                yield q != me, copy(gwd.at[s - t + piece, q], dst, 1)

    def load_start(s, cond):
        for mine, cp in weight_loads(s):
            start_if(cond & mine, [cp])

    def load_wait(s):
        slot = ring(s, 3)
        for i, buf in enumerate((wgu_b, wd_b)):
            pltpu.make_async_copy(buf.at[slot], buf.at[slot], wl_sem.at[slot, i]).wait()

    def core_copies(b):
        r, a, z = ring(b, 8), ring(b, 2), ring(b, 2)
        return (
            remote(sg.at[a, :, :, 1 - c], rdg.at[z], d_snd.at[0, r], d_rcv.at[0, r], partner),
            remote(sd.at[a, :, 1 - c], rdd.at[z], d_snd.at[1, r], d_rcv.at[1, r], partner),
        )

    def x_copies(b):
        r, a, z = ring(b, 8), ring(b, 2), ring(b, 4)
        return (
            remote(xsg.at[a], rxg.at[z], x_snd.at[0, r], x_rcv.at[0, r], x_dev),
            remote(xsd.at[a], rxd.at[z], x_snd.at[1, r], x_rcv.at[1, r], x_dev),
        )

    def y_copies(b):
        r, a, z = ring(b, 8), ring(b, 2), ring(b, 4)
        return (
            remote(ysg.at[a], ryg.at[z], y_snd.at[0, r], y_rcv.at[0, r], y_dev),
            remote(ysd.at[a], ryd.at[z], y_snd.at[1, r], y_rcv.at[1, r], y_dev),
        )

    def valid(b):
        return (b >= 0) & (b < steps)

    def start_if(cond, copies):
        for cp in copies:
            @pl.when(cond)
            def _():
                cp.start()

    def start_all(copies, b, cond=None):
        start_if(valid(b) if cond is None else valid(b) & cond, copies(b))

    def wait_all(copies, b):
        @pl.when(valid(b))
        def _():
            for cp in copies(b):
                cp.wait_recv()
            for cp in copies(b):
                cp.wait_send()

    def out_gate_up(b):
        a = ring(b, 2)
        l, m = layer_of(b), block_of(rem(b, nj))
        for gu, out in enumerate((dg_ref, du_ref)):
            for hf in range(2):
                cols = pl.ds(pl.multiple_of(hf * half + m * 128, 128), 128)
                src = fog.at[a, gu, :, pl.ds(hf * 128, 128)]
                yield pltpu.make_async_copy(src, out.at[l, :, cols], o_sem.at[a])

    def out_down(b, own):
        a, r = ring(b, 2), ring(b, 8)
        core, piece = owner_piece(rem(b, nj), c)
        dst = dd_ref.at[layer_of(b), pl.ds(pl.multiple_of(piece * 64, 64), 64)]
        if own:
            return pltpu.make_async_copy(fod.at[a], dst, f_loc.at[a])
        return remote(fod.at[a], dst, f_snd.at[r], f_rcv.at[r], partner)

    def out_start(b, cond=None):
        ok = valid(b) if cond is None else valid(b) & cond
        core, _ = owner_piece(rem(b + BASE * nj, nj), c)

        start_if(ok, out_gate_up(b))
        start_if(ok & (core == c), [out_down(b, True)])
        start_if(ok & (core != c), [out_down(b, False)])

    def out_wait(b):
        @pl.when(valid(b))
        def _():
            a = ring(b, 2)
            pltpu.make_async_copy(fog.at[a], fog.at[a], o_sem.at[a]).wait()
            core, _ = owner_piece(rem(b, nj), c)
            theirs, _ = owner_piece(rem(b, nj), 1 - c)

            @pl.when(core == c)
            def _():
                out_down(b, True).wait()

            @pl.when(core != c)
            def _():
                out_down(b, False).wait_send()

            @pl.when(theirs == c)
            def _():
                out_down(b, False).wait_recv()

    def sum_y(b):
        a, z = ring(b, 2), ring(b, 4)
        for i in range(2):
            fog[a, i] = ysg[a, i] + ryg[z, i]
        fod[a] = ysd[a] + ryd[z]

    def sum_x(b):
        a, z = ring(b, 2), ring(b, 4)
        for i in range(2):
            ysg[a, i] = pog[a, i] + rxg[z, i]
        ysd[a] = pod[a] + rxd[z]

    def sum_cores(b):
        a = ring(b, 2)
        for i in range(2):
            pog[a, i] = sg[a, i, x, c] + rdg[a, i, x]
            xsg[a, i] = sg[a, i, 1 - x, c] + rdg[a, i, 1 - x]
        pod[a] = sd[a, x, c] + rdd[a, x]
        xsd[a] = sd[a, 1 - x, c] + rdd[a, 1 - x]

    def ahead(s):
        return (s > steps - SHORT).astype(jnp.int32)

    def front(s, sent):
        sent = (next_piece(s + LEAD, sent[0]), *sent[:-1])

        @pl.when((s + 1 >= 0) & (s + 1 < steps))
        def _():
            load_wait(s + 1)

        k = ahead(s)
        wait_all(core_copies, s - 2)
        wait_all(x_copies, s - 4 + k)
        wait_all(y_copies, s - 6 + k)
        out_wait(s - 8 + k)

        full = (s >= 6) & (s < steps - SHORT)

        @pl.when(full)
        def _():
            sum_y(s - 6)
            sum_x(s - 4)
            sum_cores(s - 2)

        for f, b in ((sum_y, s - 6 + k), (sum_x, s - 4 + k)):
            @pl.when(valid(b) & ((s < 6) | (s >= steps - SHORT)))
            def _():
                f(b)

        @pl.when(s == steps - SHORT)
        def _():
            wait_all(x_copies, s - 3)
            wait_all(y_copies, s - 5)
            out_wait(s - 7)
            sum_y(s - 5)
            sum_x(s - 3)

        @pl.when(valid(s - 2) & ((s < 6) | (s >= steps - SHORT)))
        def _():
            sum_cores(s - 2)

        @pl.when(s < LEAD)
        def _():
            weights_wait(sent)

        for i, recv, send in ((2, "B", "AB"), (4, "C", "CD"), (5, "ADE", "E")):
            @pl.when((s >= LEAD) & (sent[i] > sent[i + 1]))
            def _():
                weight_wait_recv(recv, sent[i + 1])
                weight_wait_send(send, sent[i + 1])

        return sent

    def starts(s, sent, cond=None):
        k = ahead(s)

        def also(c):
            return c if cond is None else c & cond

        if cond is None:
            weights_send(sent)
        else:
            for i, kinds in ((0, "BA"), (2, "CD"), (4, "E")):
                for kind in kinds:
                    start_if(also(sent[i] > sent[i + 1]), weight_copies(kind, sent[i + 1], False))

        start_all(core_copies, s - 1, cond)
        start_all(x_copies, s - 2, cond)
        start_all(y_copies, s - 4 + k, cond)
        out_start(s - 6 + k, cond)

        load_start(s + 2, also(valid(s + 2)))
        last = s == steps - SHORT
        start_all(y_copies, s - 3, also(last))
        out_start(s - 5, also(last))

    def boundary(s, sent):
        sent = front(s, sent)
        starts(s, sent)
        return sent

    blocks = tokens // tb

    def prepare(s):
        for i in range(2):
            hb[0, i] = wgu_b[ring(s, 3), i].T

    def first(s, t):
        tok = pl.ds(t * tb, tb)
        u = dot(hb[0, 0], n_t[:, tok])
        v = dot(hb[0, 1], n_t[:, tok])
        da = dot(wd_b[ring(s, 3)], gb_t[:, tok])
        sig = jax.nn.sigmoid(u)
        silu = u * sig
        s_a[t % 2] = (silu * v).astype(BF16)
        s_du[t % 2] = (da * v * sig * (1.0 + u * (1.0 - sig))).astype(BF16)
        s_dv[t % 2] = (da * silu).astype(BF16)

    def second(s, t):
        tok = pl.ds(t * tb, tb)
        slot, w = ring(s, 2), ring(s, 3)
        for i, val in enumerate((s_du, s_dv)):
            part = dot_nt(n_t[:, tok], val[t % 2])
            if t > 0:
                part = acc[i] + part
            if t < blocks - 1:
                acc[i] = part
            else:
                sg[slot, i] = part.reshape(2, 2, dq, FB)
        part = dot_nt(gb_t[:, tok], s_a[t % 2])
        if t > 0:
            part = acc[2] + part
        if t < blocks - 1:
            acc[2] = part
        else:
            sd[slot] = part.T.reshape(2, 2, 64, width)
        dn_t[:, tok] += dot(wgu_b[w, 0], s_du[t % 2]) + dot(wgu_b[w, 1], s_dv[t % 2])

    def compute(s):
        for t in range(1, blocks):
            first(s, t)
            second(s, t - 1)
        prepare(s + 1)
        first(s + 1, 0)
        second(s, blocks - 1)

    n_tok = tokens // nb

    def tok_of(i):
        return pl.ds(pl.multiple_of(i * nb, nb), nb)

    def rows_load(i, src, which):
        return pltpu.make_async_copy(src.at[tok_of(i)], hb.at[ring(i, 2), which], hb_sem.at[ring(i, 2), which])

    def g_load(i):
        return pltpu.make_async_copy(gt_ref.at[:, tok_of(i)], acc.at[ring(i, 3)], gl_sem.at[ring(i, 3)])

    def g_store(i):
        return pltpu.make_async_copy(acc.at[ring(i, 3)], gt_ref.at[:, tok_of(i)], gs_sem.at[ring(i, 3)])

    groups = [pl.ds(k, 128) for k in range(0, width, 128)]

    def new_norm(i):
        tok = tok_of(i)
        total = jnp.zeros((1, nb), F32)
        for rows in groups:
            xt = hb[ring(i, 2), 1, :, rows].T
            n_t[rows, tok] = xt
            xf = xt.astype(F32)
            total += jnp.sum(xf * xf, axis=0, keepdims=True)
        r = lax.rsqrt(total * (1.0 / width) + EPS)
        r_row[:, tok] = r
        for rows in groups:
            n_t[rows, tok] = (n_t[rows, tok].astype(F32) * r).astype(BF16)
            dn_t[rows, tok] = jnp.zeros((128, nb), F32)

    def new_g(i, put):
        tok = tok_of(i)
        r = r_row[:, tok]
        total = jnp.zeros((1, nb), F32)
        for rows in groups:
            xt = hb[ring(i, 2), 0, :, rows].T
            gb_t[rows, tok] = xt
            total += jnp.sum(dn_t[rows, tok] * (xt.astype(F32) * r), axis=0, keepdims=True)
        m = total * (1.0 / width)
        for rows in groups:
            nf = gb_t[rows, tok].astype(F32) * r
            put(rows, acc[ring(i, 3), rows] + r * (dn_t[rows, tok] - nf * m))

    def enter_block(i):
        h_new = h_ref.at[layers - 1]

        @pl.when(i == 0)
        def _():
            rows_load(i, g_ref, 0).start()
            rows_load(i, h_new, 1).start()

        @pl.when(i + 1 < n_tok)
        def _():
            rows_load(i + 1, g_ref, 0).start()
            rows_load(i + 1, h_new, 1).start()

        @pl.when(i >= 3)
        def _():
            g_store(i - 3).wait()

        rows_load(i, g_ref, 0).wait()
        rows_load(i, h_new, 1).wait()
        for rows in groups:
            gb = hb[ring(i, 2), 0, :, rows].T
            gb_t[rows, tok_of(i)] = gb
            acc[ring(i, 3), rows] = gb.astype(F32)
        new_norm(i)
        g_store(i).start()

    def stores_done():
        for i in range(n_tok - 3, n_tok):
            g_store(i).wait()

    def between(l_new):
        h_old, h_new = h_ref.at[l_new + 1], h_ref.at[l_new]
        rows_load(0, h_old, 0).start()
        rows_load(0, h_new, 1).start()
        g_load(0).start()

        def body(i, _):
            @pl.when(i >= 2)
            def _():
                g_store(i - 2).wait()

            @pl.when(i + 1 < n_tok)
            def _():
                rows_load(i + 1, h_old, 0).start()
                rows_load(i + 1, h_new, 1).start()
                g_load(i + 1).start()

            rows_load(i, h_old, 0).wait()
            rows_load(i, h_new, 1).wait()
            g_load(i).wait()

            def put(rows, g):
                acc[ring(i, 3), rows] = g
                gb_t[rows, tok_of(i)] = g.astype(BF16)

            new_g(i, put)
            new_norm(i)
            g_store(i).start()
            return 0

        lax.fori_loop(0, n_tok, body, 0)
        for i in range(n_tok - 2, n_tok):
            g_store(i).wait()

    def leave():
        h_old = h_ref.at[0]

        def dh_store(i):
            return pltpu.make_async_copy(hb.at[ring(i, 2), 1], dh_ref.at[tok_of(i)], do_sem.at[ring(i, 2)])

        rows_load(0, h_old, 0).start()
        g_load(0).start()

        def body(i, _):
            @pl.when(i + 1 < n_tok)
            def _():
                rows_load(i + 1, h_old, 0).start()
                g_load(i + 1).start()

            @pl.when(i >= 2)
            def _():
                dh_store(i - 2).wait()

            rows_load(i, h_old, 0).wait()
            g_load(i).wait()

            def put(rows, g):
                hb[ring(i, 2), 1, :, rows] = g.astype(BF16).T

            new_g(i, put)
            dh_store(i).start()
            return 0

        lax.fori_loop(0, n_tok, body, 0)
        for i in range(n_tok - 2, n_tok):
            dh_store(i).wait()

    barrier = pltpu.get_barrier_semaphore()
    for dev in (partner, x_dev, y_dev):
        pl.semaphore_signal(barrier, inc=1, device_id=dev, device_id_type=MESH)
    pl.semaphore_wait(barrier, 3)

    per = n_tok // LEAD

    def lead_in(i, sent):
        sent = boundary(i - LEAD, sent)
        for k in range(per):
            enter_block(i * per + k)
        return sent

    sent = lax.fori_loop(0, LEAD, lead_in, (jnp.int32(0),) * 8)
    stores_done()

    def main(s, sent):
        sent = front(s, sent)
        apart = (rem(s, nj) == 0) | (s < LEAD)

        @pl.when(apart)
        def _():
            starts(s, sent)

        @pl.when(rem(s, nj) == 0)
        def _():
            @pl.when(s > 0)
            def _():
                between(layer_of(s))

            prepare(s)
            first(s, 0)

        starts(s, sent, jnp.logical_not(apart))
        compute(s)
        return sent

    sent = lax.fori_loop(0, steps, main, sent)
    sent = lax.fori_loop(steps, steps + 2, boundary, sent)
    leave()
    lax.fori_loop(steps + 2, steps + 7, boundary, sent)


def backward(dims, h, g, gate, up, wd):
    layers, tokens, width, hidden, tb, nb = dims
    dq = width // 4
    nj = hidden // FB
    steps = layers * nj
    dma = pltpu.SemaphoreType.DMA
    vm = pltpu.VMEM
    anyspace = pl.BlockSpec(memory_space=pl.ANY)
    sds = jax.ShapeDtypeStruct
    out_shape = [
        sds((layers, dq, hidden), F32),
        sds((layers, dq, hidden), F32),
        sds((layers, hidden // 4, width), F32),
        sds((tokens, width), BF16),
        sds((steps, 4, 2, dq, FB), BF16),
        sds((steps, 4, 64, width), BF16),
        sds((width, tokens), F32),
    ]

    def pair(n):
        return [vm((n, 2, dq, FB), F32), vm((n, 64, width), F32)]

    scratch = [
        vm((width, tokens), BF16),
        vm((width, tokens), BF16),
        vm((width, tokens), F32),
        vm((1, tokens), F32),
        vm((3, 2, width, FB), BF16),
        vm((3, FB, width), BF16),
        vm((2, FB, tb), BF16),
        vm((2, FB, tb), BF16),
        vm((2, FB, tb), BF16),
        vm((3, width, FB), F32),
        vm((2, 2, nb, width), BF16),
        vm((2, 2, 2, 2, dq, FB), F32),
        vm((2, 2, 2, 64, width), F32),
        vm((2, 2, 2, dq, FB), F32),
        vm((2, 2, 64, width), F32),
        *pair(2), *pair(2), *pair(4), *pair(2), *pair(4), *pair(2),
        dma((3, 2)),
        dma((2, 8)), dma((2, 8)), dma((2, 8)), dma((2, 8)), dma((2, 8)), dma((2, 8)),
        dma((2,)), dma((2,)), dma((8,)), dma((8,)),
        dma((5, 2, RS)), dma((5, 2, RS)),
        dma((2, 2)), dma((3,)), dma((3,)), dma((2,)),
    ]
    return pl.pallas_call(
        functools.partial(kernel, dims),
        out_shape=out_shape,
        in_specs=[anyspace] * 5,
        out_specs=[anyspace] * 7,
        scratch_shapes=scratch,
        compiler_params=pltpu.CompilerParams(
            collective_id=0, has_side_effects=True, vmem_limit_bytes=67043328,
        ),
        name="mlp_backward",
    )(h, g, gate, up, wd)[:4]


def solution(mesh):
    tok_spec = P(("dp", "fsdp"))
    stack_spec = P(None, ("dp", "fsdp"))
    weight_spec = P(None, "fsdp")

    def local_backward(h_saved, grad_out, gate_sh, up_sh, down_sh):
        layers = h_saved.shape[0]
        b_loc, seq, width = grad_out.shape
        tokens = b_loc * seq
        dq, hidden = gate_sh.shape[1:]
        nj = hidden // FB
        tb = min(512, tokens // 2)
        nb = FB
        wd = down_sh.reshape(layers, nj, 64, width)
        dims = (layers, tokens, width, hidden, tb, nb)
        d_gate, d_up, d_down, d_h0 = backward(
            dims, h_saved.reshape(layers, tokens, width), grad_out.reshape(tokens, width), gate_sh, up_sh, wd
        )
        return d_gate, d_up, d_down, d_h0.reshape(b_loc, seq, width)

    return jax.shard_map(
        local_backward,
        mesh=mesh,
        in_specs=(stack_spec, tok_spec, weight_spec, weight_spec, weight_spec),
        out_specs=(weight_spec, weight_spec, weight_spec, tok_spec),
        check_vma=False,
    )
```
